128 devices in a mesh: patch: 16 (over y, z), hidden: 8 (over x, core).
Axes of the slice: x: 4, y: 4, z: 4, core: 2. Of those that a mesh axis runs over, the one named last changes fastest.
Arguments:
- grid_latent: bfloat16 [49152, 512], P('patch'), may hold values from -6 to 6
- mesh_latent: bfloat16 [81920, 512], P('patch'), may hold values from -6 to 6
- edge_latent: bfloat16 [131072, 512], P('patch'), may hold values from -6 to 6
- senders: int32 [131072], P('patch'), may hold values from 0 to 49151, as said below
- receivers: int32 [131072], P('patch'), may hold values from 0 to 81919
- mesh_slot: int32 [81920], replicated, may hold values from 0 to 81919, as said below
- edge_counts: int32 [16], P('patch'), may hold values from 2730 to 8192, as said below
- w_edge: bfloat16 [512, 512], P(None, 'hidden'), may hold values from -0.25 to 0.25
- w_sender: bfloat16 [512, 512], P(None, 'hidden'), may hold values from -0.25 to 0.25
- w_receiver: bfloat16 [512, 512], P(None, 'hidden'), may hold values from -0.25 to 0.25
- edge_bias: float32 [512], P('hidden'), may hold values from -3 to 3
- w_edge_out: bfloat16 [512, 512], P('hidden'), may hold values from -0.25 to 0.25
- edge_out_bias: float32 [512], P('hidden'), may hold values from -3 to 3
- edge_gain: float32 [512], P('hidden'), may hold values from 0.25 to 1.75
- edge_shift: float32 [512], P('hidden'), may hold values from -2 to 2
- w_mesh_in: bfloat16 [512, 512], P(None, 'hidden'), may hold values from -0.25 to 0.25
- w_message_in: bfloat16 [512, 512], P(None, 'hidden'), may hold values from -0.25 to 0.25
- mesh_bias: float32 [512], P('hidden'), may hold values from -3 to 3
- w_mesh_out: bfloat16 [512, 512], P('hidden'), may hold values from -0.25 to 0.25
- mesh_out_bias: float32 [512], P('hidden'), may hold values from -3 to 3
- mesh_gain: float32 [512], P('hidden'), may hold values from 0.25 to 1.75
- mesh_shift: float32 [512], P('hidden'), may hold values from -2 to 2
Outputs:
- mesh_out: bfloat16 [81920, 512], P('patch', 'hidden')
- edge_out: bfloat16 [131072, 512], P('patch', 'hidden')
The draws below stay inside these ranges and needn't reach their ends.
Inputs may be any that keep to these rules, and one draw needn't show every extreme that they name: `mesh_slot`: A permutation of the mesh node ids 0 to 81919; owner block p holds mesh rows p * 5120 to (p + 1) * 5120 - 1. `senders`: edge slots of block p (slots p * 8192 to (p + 1) * 8192 - 1) send from grid nodes p * 3072 to (p + 1) * 3072 - 1. Only the first edge_counts[p] slots of block p are live; some block is full.
All inputs are finite; a program needn't handle non-finite values.
Results may differ from the reference program's by a relative error of at most 0.014.
Values may be sent and summed in bfloat16 or wider, within the bound.
No kernel may reach another device: no remote copies, remote signals or barrier semaphores. Data moves between devices by JAX's collectives and lax.ppermute only.
A program may use at most 192 MiB of HBM per device.

```python
import jax
import jax.numpy as jnp
from jax import lax

LATENT = 512
G_DEV = 3072
E_DEV = 8192
MESH_DEV = 5120
GRID = 49152
EDGES = 131072
MESH = 81920
N_HIDDEN = 8


def mesh_order(key):
    return jax.random.permutation(jax.random.fold_in(key, 11), MESH).astype(jnp.int32)


def draw_mesh_slot(key, part):
    return mesh_order(key)


def draw_receivers(key, part):
    order = mesh_order(key)
    inverse = jnp.argsort(order, stable=True).astype(jnp.int32)
    first, second = jax.random.split(jax.random.fold_in(key, 12))
    third = jax.random.fold_in(key, 15)
    position = jnp.arange(EDGES, dtype=jnp.int32)
    blocks = EDGES // E_DEV
    pick = jax.random.randint(first, (EDGES,), 0, 8)
    anywhere = jax.random.randint(third, (EDGES,), 0, blocks).astype(jnp.int32)
    offset = jnp.where(pick == 4, -1, jnp.where(pick == 7, 1, 0)).astype(jnp.int32)
    nearby = (position // E_DEV + offset + blocks) % blocks
    owner = jnp.where(pick < 4, anywhere, nearby).astype(jnp.int32)
    target = owner * MESH_DEV + jax.random.randint(second, (EDGES,), 0, MESH_DEV)
    return jnp.take(inverse, target).astype(jnp.int32)


def draw_senders(key, part):
    position = jnp.arange(EDGES, dtype=jnp.int32)
    local = jax.random.randint(jax.random.fold_in(key, 13), (EDGES,), 0, G_DEV)
    return (position // E_DEV * G_DEV + local).astype(jnp.int32)


def draw_edge_counts(key, part):
    first, second = jax.random.split(jax.random.fold_in(key, 14))
    blocks = EDGES // E_DEV
    counts = jax.random.randint(first, (blocks,), E_DEV // 3, E_DEV + 1)
    fullest = jax.random.randint(second, (), 0, blocks)
    return jnp.where(jnp.arange(blocks) == fullest, E_DEV, counts).astype(jnp.int32)


def steps_of(own_key, extent, shards, smallest, high):
    level, own = 1.0, jax.random.fold_in(own_key, 6)
    for axis_at, shards_of in shards:
        heights = jnp.exp(jax.random.uniform(jax.random.fold_in(own, axis_at), (shards_of,), jnp.float32, smallest / len(shards), high / len(shards)))
        level = level * jnp.repeat(heights, extent[axis_at] // shards_of).reshape([-1 if axis == axis_at else 1 for axis in range(len(extent))])
    return level


def bell_draw(rng, extent, scale, most, shards=(), held_as=jnp.bfloat16):
    entries = scale * jax.random.normal(rng, extent, jnp.float32)
    if shards:
        entries = entries * steps_of(rng, extent, shards, -0.22, 0.18)
    return jnp.clip(entries, -most, most).astype(held_as)


def setup_inputs(seed: int = 0) -> dict:
    key_list = jax.random.split(jax.random.key(seed), 23)
    return {
        "grid_latent": bell_draw(key_list[0], (GRID, LATENT), 1.0, 6.0, ((0, 16),)),
        "mesh_latent": bell_draw(key_list[1], (MESH, LATENT), 1.0, 6.0, ((0, 16),)),
        "edge_latent": bell_draw(key_list[2], (EDGES, LATENT), 1.0, 6.0, ((0, 16),)),
        "senders": draw_senders(jax.random.fold_in(key_list[22], 71), 0),
        "receivers": draw_receivers(jax.random.fold_in(key_list[22], 71), 0),
        "mesh_slot": draw_mesh_slot(jax.random.fold_in(key_list[22], 71), 0),
        "edge_counts": draw_edge_counts(jax.random.fold_in(key_list[22], 71), 0),
        "w_edge": bell_draw(key_list[7], (LATENT, LATENT), LATENT ** -0.5, 0.25, ((1, 8),)),
        "w_sender": bell_draw(key_list[8], (LATENT, LATENT), LATENT ** -0.5, 0.25, ((1, 8),)),
        "w_receiver": bell_draw(key_list[9], (LATENT, LATENT), LATENT ** -0.5, 0.25, ((1, 8),)),
        "edge_bias": bell_draw(key_list[10], (LATENT,), 0.5, 3.0, ((0, 8),), jnp.float32),
        "w_edge_out": bell_draw(key_list[11], (LATENT, LATENT), LATENT ** -0.5, 0.25, ((0, 8),)),
        "edge_out_bias": bell_draw(key_list[12], (LATENT,), 0.5, 3.0, ((0, 8),), jnp.float32),
        "edge_gain": jnp.clip(1.0 + 0.15 * jax.random.normal(key_list[13], (LATENT,), jnp.float32), 0.25, 1.75),
        "edge_shift": bell_draw(key_list[14], (LATENT,), 0.3, 2.0, ((0, 8),), jnp.float32),
        "w_mesh_in": bell_draw(key_list[15], (LATENT, LATENT), LATENT ** -0.5, 0.25, ((1, 8),)),
        "w_message_in": bell_draw(key_list[16], (LATENT, LATENT), LATENT ** -0.5, 0.25, ((1, 8),)),
        "mesh_bias": bell_draw(key_list[17], (LATENT,), 0.5, 3.0, ((0, 8),), jnp.float32),
        "w_mesh_out": bell_draw(key_list[18], (LATENT, LATENT), LATENT ** -0.5, 0.25, ((0, 8),)),
        "mesh_out_bias": bell_draw(key_list[19], (LATENT,), 0.5, 3.0, ((0, 8),), jnp.float32),
        "mesh_gain": jnp.clip(1.0 + 0.15 * jax.random.normal(key_list[20], (LATENT,), jnp.float32), 0.25, 1.75),
        "mesh_shift": bell_draw(key_list[21], (LATENT,), 0.3, 2.0, ((0, 8),), jnp.float32),
    }


def group_sum(hidden_units, w_out):
    width = w_out.shape[0] // N_HIDDEN
    total = jnp.zeros((hidden_units.shape[0], w_out.shape[1]), jnp.float32)
    for group in range(N_HIDDEN):
        part = jnp.dot(hidden_units[:, group * width:(group + 1) * width], w_out[group * width:(group + 1) * width], preferred_element_type=jnp.float32)
        part = lax.optimization_barrier(part.astype(jnp.bfloat16))
        total = total + part.astype(jnp.float32)
    return total

def normalize(values, gain, offset):
    center = lax.optimization_barrier(jnp.mean(values, axis=1, keepdims=True))
    centered = values - center
    spread = lax.optimization_barrier(jnp.mean(centered * centered, axis=1, keepdims=True))
    return centered * lax.rsqrt(spread + 1e-05) * gain + offset

def reference(grid_latent, mesh_latent, edge_latent, senders, receivers, mesh_slot, edge_counts, w_edge, w_sender, w_receiver, edge_bias, w_edge_out, edge_out_bias, edge_gain, edge_shift, w_mesh_in, w_message_in, mesh_bias, w_mesh_out, mesh_out_bias, mesh_gain, mesh_shift):
    target = jnp.take(mesh_slot, receivers).astype(jnp.int32)
    position = jnp.arange(EDGES, dtype=jnp.int32)
    live = (position % E_DEV < jnp.take(edge_counts, position // E_DEV)).astype(jnp.float32)
    receiver_proj = jnp.dot(mesh_latent, w_receiver, preferred_element_type=jnp.float32).astype(jnp.bfloat16)
    sender_proj = jnp.dot(grid_latent, w_sender, preferred_element_type=jnp.float32)
    edge_pre = jnp.dot(edge_latent, w_edge, preferred_element_type=jnp.float32)
    edge_pre = edge_pre + jnp.take(sender_proj, senders, axis=0) + jnp.take(receiver_proj, target, axis=0).astype(jnp.float32) + edge_bias
    edge_hidden = jax.nn.silu(edge_pre).astype(jnp.bfloat16)
    edge_sum = group_sum(edge_hidden, w_edge_out) + edge_out_bias
    message = normalize(edge_sum, edge_gain, edge_shift) * live[:, None]
    edge_out = (edge_latent.astype(jnp.float32) + message).astype(jnp.bfloat16)
    summed = jax.ops.segment_sum(message, target, num_segments=MESH).astype(jnp.bfloat16)
    mesh_pre = jnp.dot(mesh_latent, w_mesh_in, preferred_element_type=jnp.float32) + jnp.dot(summed, w_message_in, preferred_element_type=jnp.float32) + mesh_bias
    mesh_hidden = jax.nn.silu(mesh_pre).astype(jnp.bfloat16)
    mesh_sum = group_sum(mesh_hidden, w_mesh_out) + mesh_out_bias
    mesh_out = (mesh_latent.astype(jnp.float32) + normalize(mesh_sum, mesh_gain, mesh_shift)).astype(jnp.bfloat16)
    return (mesh_out, edge_out)
```

```python
import jax
import jax.numpy as jnp
from jax import lax
from jax.experimental import pallas as pl
from jax.experimental.pallas import tpu as pltpu
from jax.sharding import PartitionSpec as P


EPSILON = 1e-05
LANES = 128
BF = jnp.bfloat16
F32 = jnp.float32
I32 = jnp.int32

NP = 16
NH = 8
D = 512
E = 8192
G = 3072
M = 5120
ML = M // NH
ROWS = E // LANES
N1 = 1152
HALF = N1 // 2
CA = 64
CX = 160
CS = 384
FLAG = 16
OUT_ROWS = HALF + FLAG
OP = NP * CA
OM = OP + 256
OS = OM + 256
NS = OS + CS
WIN = 64
VROW = 128
WROWS = VROW + 8
STEP = 128
VMEM = 60 * 1024 * 1024


def dot(a, b):
    return jnp.dot(a, b, preferred_element_type=F32)


def dot_nt(a, b):
    return lax.dot_general(a, b, (((1,), (1,)), ((), ())), preferred_element_type=F32)


def iota(shape, axis):
    return lax.broadcasted_iota(I32, shape, axis)


def onehot(cond):
    return jnp.where(cond, 1.0, 0.0).astype(BF)


def lane_join(a, b):
    low = iota(a.shape, 1) < 64
    return jnp.where(low, a, pltpu.roll(b, 64, 1)), jnp.where(low, pltpu.roll(a, 64, 1), b)


def silu(v):
    return v / (1.0 + jnp.exp(-v))


def normalized(v, gain, shift):
    mean = jnp.mean(v, axis=1, keepdims=True)
    c = v - mean
    var = jnp.mean(c * c, axis=1, keepdims=True)
    return c * lax.rsqrt(var + EPSILON) * gain + shift


def row_of(x):
    return jnp.concatenate([x[i : i + 1, :] for i in range(x.shape[0])], axis=1)


def gather_kernel(
    count_ref, where_ref, recv_ref, slots_ref, send_ref, edge_hbm, grid_hbm,
    key_ref, starts_ref, list_ref, sent_ref, info_ref, slot_ref, slot_row_ref,
    table, tgt, hits, starts, edge, grid, acc, meta, edge_sem, grid_sem, starts_sem,
):
    chunk = lambda i: pltpu.make_async_copy(
        edge_hbm.at[pl.ds(i * 1024, 1024)], edge.at[pl.ds(i * 1024, 1024)], edge_sem.at[i]
    )
    for i in range(8):
        chunk(i).start()
    grid_copy = pltpu.make_async_copy(grid_hbm, grid, grid_sem)
    grid_copy.start()
    own = where_ref[0]
    patch = where_ref[1]
    v = slots_ref[...]
    table[:, 0:128] = ((v >> 8) - 160).astype(F32).astype(BF)
    table[:, 128:256] = (v & 255).astype(F32).astype(BF)

    def group(g, carry):
        r = recv_ref[pl.ds(pl.multiple_of(g * 8, 8), 8), :]
        hi = (r >> 7).astype(F32).T
        lo = (r & 127).astype(F32).T
        rows = iota((128, 640), 1).astype(F32)
        for j in range(8):
            hits[128 * j : 128 * j + 128, :] = onehot(rows == hi[:, j : j + 1])
        y = dot(hits[...], table[...])
        full = (y[:, 0:128] + 160.0) * 256.0 + y[:, 128:256]
        lane = iota((128, 128), 1).astype(F32)
        which = iota((128, 8), 1)
        got = jnp.zeros((128, 8), F32)
        for j in range(8):
            part = jnp.where(lane == lo[:, j : j + 1], full[128 * j : 128 * j + 128], 0.0)
            got = jnp.where(which == j, jnp.sum(part, axis=1, keepdims=True), got)
        tgt[pl.ds(pl.multiple_of(g * 8, 8), 8), :] = got.T
        return carry

    lax.fori_loop(0, ROWS // 8, group, 0)
    t = tgt[...]
    block = jnp.floor((t + 0.5) * (1.0 / ML))
    l = t - block * ML
    q = jnp.floor((block + 0.5) * (1.0 / NH))
    h = block - q * NH
    position = iota((ROWS, 128), 0) * 128 + iota((ROWS, 128), 1)
    live = position < count_ref[0]
    upper = onehot(iota((128, 128), 0) < iota((128, 128), 1))
    big = NH * ROWS
    row, col = iota((big, big), 0), iota((big, big), 1)
    lower = onehot((col < row) & ((col >> 6) == (row >> 6)))
    mine = [live & (h == float(k)) for k in range(NH)]
    mask = jnp.concatenate([onehot(m) for m in mine], axis=0)
    before_all = dot(mask, upper)
    counts_all = dot(mask, jnp.ones((128, 128), BF))
    above_all = dot(lower, counts_all.astype(BF))
    c = jnp.full((ROWS, 128), -1.0, F32)
    delta = jnp.full((ROWS, 128), -1.0, F32)
    begin = jnp.zeros((ROWS, 128), F32)
    totals = jnp.zeros((8, 128), F32)
    lane64 = iota((ROWS, 128), 1)
    lane8 = iota((8, 128), 1)
    for k in range(NH):
        at = slice(ROWS * k, ROWS * k + ROWS)
        above = above_all[at]
        place = before_all[at] + above
        start = jnp.floor(above * (1.0 / 16.0)) * 16.0
        c = jnp.where(mine[k], place, c)
        delta = jnp.where(mine[k], place - start, delta)
        begin = jnp.where(lane64 == k, start, begin)
        total = above[ROWS - 1 : ROWS, :] + counts_all[at][ROWS - 1 : ROWS, :]
        totals = jnp.where(lane8 == k, total, totals)
    key_ref[...] = jnp.where(delta >= 0.0, h * 256.0 + delta, -1.0)
    starts_ref[0:ROWS, :] = begin.astype(I32)
    spread = jnp.where(jnp.max(delta) >= WIN, 1.0, 0.0)
    starts_ref[ROWS : ROWS + 8, :] = totals.astype(I32)
    to_scalars = pltpu.make_async_copy(starts_ref, starts, starts_sem)
    to_scalars.start()
    acc[...] = jnp.zeros_like(acc)
    meta[...] = jnp.zeros_like(meta)
    s = (send_ref[...] - patch * G).astype(F32)
    s_hi = jnp.floor(s * (1.0 / 256.0))
    l_hi = jnp.floor(l * (1.0 / 256.0))
    kinds = [s_hi, s - 256.0 * s_hi, q, l_hi, l - 256.0 * l_hi, jnp.ones((ROWS, 128), F32)]
    c = jnp.where(h == own.astype(F32), c, -1.0)
    to_scalars.wait()
    total = starts[ROWS, own]
    for i in range(16):
        if i % 2 == 0:
            chunk(i // 2).wait()
        at4 = slice(4 * i, 4 * i + 4)
        c_row = row_of(c[at4])
        facts = jnp.concatenate([row_of(x[at4]) for x in kinds] + [jnp.zeros((2, 512), F32)], axis=0).astype(BF)

        def add(at, i=i, c_row=c_row, facts=facts):
            hit = onehot(c_row == (iota((STEP, 512), 0) + at).astype(F32))
            acc[pl.ds(at, STEP), :] += dot(hit, edge[512 * i : 512 * i + 512, :])
            meta[pl.ds(at, STEP), :] += dot_nt(hit, facts)

        first = starts[4 * i, own]
        last = total if i == 15 else starts[4 * i + 4, own] + 16
        rounds = (jnp.minimum(last, N1) - first + STEP - 1) // STEP
        add(pl.multiple_of(jnp.minimum(first, N1), 16))

        def more(k, carry, first=first, add=add):
            add(pl.multiple_of(first + STEP * k, 16))
            return carry

        lax.fori_loop(1, rounds, more, 0)
    grid_copy.wait()
    carry = jnp.zeros((1, 128), F32)
    bad = jnp.maximum(jnp.where(total > N1, 1.0, 0.0), spread)
    T = 384
    lower = onehot(iota((T, T), 1) < iota((T, T), 0))
    for i in range(N1 // T):
        at = slice(T * i, T * i + T)
        facts = meta[at, :]
        valid = facts[:, 5:6] > 0.5
        sender = jnp.where(valid, facts[:, 0:1] * 256.0 + facts[:, 1:2], -1.0)
        hit = onehot(iota((T, G), 1).astype(F32) == sender)
        sent_ref[at, :] = dot(hit, grid[...]).astype(BF)
        list_ref[at, :] = acc[at, :].astype(BF)
        lane = iota((T, 128), 1)
        info = jnp.where(lane == 0, facts[:, 3:4], jnp.where(lane == 1, facts[:, 4:5], 0.0))
        info_ref[at, :] = jnp.where(lane == 2, 1.0, info).astype(BF)
        owner = jnp.where((lane.astype(F32) == facts[:, 2:3]) & valid, 1.0, 0.0)
        rank = jnp.sum(owner * (dot(lower, owner.astype(BF)) + carry), axis=1, keepdims=True)
        carry = carry + jnp.sum(owner, axis=0, keepdims=True)
        d = facts[:, 2:3] - patch.astype(F32)
        d = jnp.where(d < 0.0, d + NP, d)
        more = rank - CA
        slot = jnp.where((d == 1.0) & (more < CX), OP + more, -1.0)
        slot = jnp.where((d == NP - 1.0) & (more < CX), OM + more, slot)
        slot = jnp.where(rank < CA, facts[:, 2:3] * CA + rank, slot)
        slot = jnp.where(d == 0.0, jnp.where(rank < CS, OS + rank, -1.0), slot)
        bad = jnp.maximum(bad, jnp.max(jnp.where(valid & (slot < 0.0), 1.0, 0.0)))
        slots = jnp.broadcast_to(jnp.where(valid, slot, -1.0), (T, 128))
        slot_ref[at, :] = slots[:, 0:8]
        slot_row_ref[:, at] = slots.T[0:8, :]
    slot_row_ref[:, N1 : N1 + 128] = jnp.broadcast_to(bad, (8, 128))


def gather(count, where, receivers, mesh_slot, senders, edge_latent, grid_latent):
    sds = jax.ShapeDtypeStruct
    smem = pl.BlockSpec(memory_space=pltpu.SMEM)
    vmem = pl.BlockSpec(memory_space=pltpu.VMEM)
    hbm = pl.BlockSpec(memory_space=pl.ANY)
    return pl.pallas_call(
        gather_kernel,
        out_shape=(
            sds((ROWS, 128), F32), sds((ROWS + 8, 128), I32),
            sds((N1, D), BF), sds((N1, D), BF), sds((N1, 128), BF), sds((N1, 8), F32), sds((8, N1 + 128), F32),
        ),
        in_specs=[smem, smem, vmem, vmem, vmem, hbm, hbm],
        scratch_shapes=[
            pltpu.VMEM((640, 256), BF),
            pltpu.VMEM((ROWS, 128), F32),
            pltpu.VMEM((1024, 640), BF),
            pltpu.SMEM((ROWS + 8, 128), I32),
            pltpu.VMEM((E, D), BF),
            pltpu.VMEM((G, D), BF),
            pltpu.VMEM((N1 + STEP, D), F32),
            pltpu.VMEM((N1 + STEP, 8), F32),
            pltpu.SemaphoreType.DMA((8,)),
            pltpu.SemaphoreType.DMA(()),
            pltpu.SemaphoreType.DMA(()),
        ],
        compiler_params=pltpu.CompilerParams(vmem_limit_bytes=VMEM),
        name="gather",
    )(
        count, where, receivers.reshape(ROWS, 128), mesh_slot.reshape(640, 128), senders.reshape(ROWS, 128),
        edge_latent, grid_latent,
    )


def walk_of(own):
    x, core = own // 2, own % 2
    places = [2 * ((x + 4 - k) % 4) for k in range(4)]
    return [p + core for p in places] + [p + 1 - core for p in places]


def vectors_of(v_ref, m, order=tuple(range(NH))):
    pairs = []
    for k in range(NH // 2):
        at = slice(128 * m, 128 * m + 128)
        x, y = v_ref[order[2 * k], :, at].astype(F32), v_ref[order[2 * k + 1], :, at].astype(F32)
        pairs.append(lane_join(x, y))
    rows = [jnp.concatenate([p[i] for p in pairs], axis=1) for i in range(2)]
    return [r[0:1] + r[1:2] + r[2:3] for r in rows]


def stack_kernel(e, s, r, mi, mm, eo, mo, *refs):
    vectors, (first_ref, second_ref) = refs[:8], refs[8:]
    for k, w in enumerate((r, mi, mm, eo, mo)):
        second_ref[64 * k : 64 * k + 64, :] = w[...]
    v = jnp.concatenate([x[...] for x in vectors], axis=1)
    v = jnp.broadcast_to(v, (8, D))
    hi = v.astype(BF)
    v = v - hi.astype(F32)
    mid = v.astype(BF)
    low = (v - mid.astype(F32)).astype(BF)
    row = iota((8, D), 0)
    parts = jnp.where(row == 0, hi.astype(F32), jnp.where(row == 1, mid.astype(F32), low.astype(F32)))
    parts = jnp.where(row < 3, parts, 0.0).astype(BF)
    for n in range(NH):
        first_ref[n, 0:64, :] = e[...]
        first_ref[n, 64:128, :] = s[...]
        first_ref[n, VROW:WROWS, :] = parts


def stacked(*args):
    return pl.pallas_call(
        stack_kernel,
        out_shape=(jax.ShapeDtypeStruct((NH, WROWS, D), BF), jax.ShapeDtypeStruct((320, D), BF)),
        name="stacked",
    )(*args)


def to_all(first, second):
    first = lax.all_to_all(first, "hidden", split_axis=0, concat_axis=0, tiled=True)
    walk = [second]
    for k in (1, 2, 3):
        walk.append(lax.ppermute(second, "hidden", [(i, (i + 2 * k) % NH) for i in range(NH)]))
    walk = jnp.stack(walk)
    other = lax.ppermute(walk, "hidden", [(i, i ^ 1) for i in range(NH)])
    return first, walk, other


def pack_kernel(where_ref, list_ref, sent_ref, info_ref, slot_row_ref, first_ref, oa_ref, op_ref, om_ref, pre, wide):
    order = walk_of(where_ref[0])
    w_edge = jnp.concatenate([first_ref[n, 0:64, :] for n in order], axis=0)
    w_sender = jnp.concatenate([first_ref[n, 64:128, :] for n in order], axis=0)
    bias = vectors_of(first_ref.at[:, VROW:WROWS], 0, order)[0]
    T = 384
    for i in range(N1 // T):
        at = slice(T * i, T * i + T)
        pre[at, 0:D] = (dot_nt(list_ref[at, :], w_edge) + dot_nt(sent_ref[at, :], w_sender) + bias).astype(BF)
    pre[:, D : D + 128] = info_ref[...]
    for i in range(OS // T):
        hit = onehot((iota((T, N1), 0) + T * i).astype(F32) == slot_row_ref[0:1, 0:N1])
        wide[T * i : T * i + T, :] = dot(hit, pre[...])
    kind = iota((8, 128), 0)
    bad = slot_row_ref[0:8, N1 : N1 + 128]

    def facts_of(at):
        return jnp.where(kind == 3, bad, wide[at : at + 128, D : D + 128].T[0:8, :])

    for i in range(NP // 2):
        x = facts_of(128 * i)
        low = iota((8, 128), 1) < 64
        turned = pltpu.roll(x, 64, 1)
        for odd in range(2):
            n = 2 * i + odd
            oa_ref[n, 0:CA, :] = wide[CA * n : CA * n + CA, 0:D].astype(BF)
            both = jnp.where(low, turned, x) if odd else jnp.where(low, x, turned)
            oa_ref[n, CA : CA + 8, :] = jnp.zeros((8, D), BF)
            oa_ref[n, CA : CA + 8, 0:128] = both.astype(BF)
    for ref, at, size in ((op_ref, OP, CX), (om_ref, OM, CX)):
        ref[0:size, :] = wide[at : at + size, 0:D].astype(BF)
        ref[size : size + 8, :] = jnp.zeros((8, D), BF)
        for k in range((size + 127) // 128):
            ref[size : size + 8, 128 * k : 128 * k + 128] = facts_of(at + 128 * k).astype(BF)


def pack(where, edges, sent, info, slot_row, first):
    sds = jax.ShapeDtypeStruct
    fixed = lambda *shape: pl.BlockSpec(shape, lambda b: (0,) * len(shape))
    shapes = ((NP, CA + 8, D), (CX + 8, D), (CX + 8, D), (N1, D + 128))
    return pl.pallas_call(
        pack_kernel,
        grid=(1,),
        in_specs=[pl.BlockSpec(memory_space=pltpu.SMEM)]
        + [fixed(N1, D), fixed(N1, D), fixed(N1, 128), fixed(8, N1 + 128), fixed(NH, WROWS, D)],
        out_specs=tuple(fixed(*x) for x in shapes),
        out_shape=tuple(sds(x, BF) for x in shapes),
        scratch_shapes=[pltpu.VMEM((OS, D + 128), F32)],
        compiler_params=pltpu.CompilerParams(vmem_limit_bytes=VMEM),
        name="pack",
    )(where, edges, sent, info, slot_row, first)


def full(w_refs):
    return jnp.concatenate([w[...].reshape(D // 2, D) for w in w_refs], axis=0)


def weight_specs(*which):
    one = lambda k: pl.BlockSpec((NH // 2, 64, D), lambda *_: (0, k, 0))
    vec = pl.BlockSpec((NH, 8, D), lambda *_: (0, VROW // 8, 0))
    return [one(k) for k in which for _ in range(2)] + [vec]


def messages(x, l, proj, w_out, vec):
    hit = onehot(iota((x.shape[0], ML), 1).astype(F32) == l)
    hidden = silu(x + dot(hit, proj)).astype(BF)
    message = normalized(dot(hidden, w_out) + vec[0], vec[1], vec[2])
    return jnp.where(l >= 0.0, message, 0.0).astype(BF)


def edge_vectors(v_ref):
    return vectors_of(v_ref, 1) + vectors_of(v_ref, 2)[0:1]


def local_kernel(where_ref, pre_ref, slot_row_ref, mesh_ref, wr_ref, wr2_ref, wo_ref, wo2_ref, v_ref, proj_ref, msg_ref, l_ref):
    proj = dot_nt(mesh_ref[...], full((wr_ref, wr2_ref))).astype(BF)
    proj_ref[...] = proj
    hit = onehot((iota((CS, N1), 0) + OS).astype(F32) == slot_row_ref[0:1, 0:N1])
    x = dot(hit, pre_ref[...])
    l = jnp.where(x[:, D + 2 : D + 3] > 0.5, x[:, D : D + 1] * 256.0 + x[:, D + 1 : D + 2], -1.0)
    msg_ref[...] = messages(x[:, 0:D], l, proj_ref[...], full((wo_ref, wo2_ref)), edge_vectors(v_ref))
    l_ref[...] = jnp.broadcast_to(l, (CS, 128)).T[0:8, :]


def local(where, pre, slot_row, mesh_latent, weights):
    first, walk, other = weights
    sds = jax.ShapeDtypeStruct
    fixed = lambda *shape: pl.BlockSpec(shape, lambda b, w: (0,) * len(shape))
    return pl.pallas_call(
        local_kernel,
        grid_spec=pltpu.PrefetchScalarGridSpec(
            num_scalar_prefetch=1,
            grid=(1,),
            in_specs=[
                fixed(N1, D + 128), fixed(8, N1 + 128),
                pl.BlockSpec((ML, D), lambda b, w: (w[0], 0)),
            ] + weight_specs(0, 3),
            out_specs=(fixed(ML, D), fixed(CS, D), fixed(8, CS)),
        ),
        out_shape=(sds((ML, D), BF), sds((CS, D), BF), sds((8, CS), F32)),
        compiler_params=pltpu.CompilerParams(vmem_limit_bytes=VMEM),
        name="local",
    )(where, pre, slot_row, mesh_latent, walk, other, walk, other, first)


def owner_kernel(
    ra_ref, rp_ref, rm_ref, proj_ref, wo_ref, wo2_ref, v_ref,
    oa_ref, op_ref, om_ref, l_row_ref, flag_ref,
    x_s, l_col,
):
    low = iota((8, 128), 1) < 64
    flags = jnp.zeros((8, 128), F32)
    pieces = []
    for i in range(NP // 2):
        a = ra_ref[2 * i, CA : CA + 8, 0:128].astype(F32)
        b = ra_ref[2 * i + 1, CA : CA + 8, 0:128].astype(F32)
        pieces.append(jnp.where(low, a, b))
    for ref, size in ((rp_ref, CX), (rm_ref, CX)):
        for k in range((size + 127) // 128):
            pieces.append(ref[size : size + 8, 128 * k : 128 * k + 128].astype(F32))
    for k, m in enumerate(pieces):
        flags = jnp.maximum(flags, m)
        l = jnp.where(m[2:3] > 0.5, m[0:1] * 256.0 + m[1:2], -1.0)
        l = jnp.broadcast_to(l, (8, 128))
        l_row_ref[:, 128 * k : 128 * k + 128] = l
        l_col[128 * k : 128 * k + 128, :] = l.T
    flag_ref[...] = jnp.broadcast_to(flags[3:4], (8, 128))
    for n in range(NP):
        x_s[CA * n : CA * n + CA, :] = ra_ref[n, 0:CA, :]
    for ref, at in ((rp_ref, OP), (rm_ref, OM)):
        x_s[at : at + CX, :] = ref[0:CX, :]
        x_s[at + CX : at + 256, :] = jnp.zeros((256 - CX, D), BF)
    vec = edge_vectors(v_ref)
    w_out = full((wo_ref, wo2_ref))
    T = 256
    for i in range(OS // T):
        at = slice(T * i, T * i + T)
        got = messages(x_s[at, :].astype(F32), l_col[at, 0:1], proj_ref[...], w_out, vec)
        if i < OP // T:
            for n in range(T // CA):
                oa_ref[T // CA * i + n, :, :] = got[CA * n : CA * n + CA]
        else:
            (op_ref if i == OP // T else om_ref)[...] = got[0:CX]


def owner(ra, rp, rm, proj, weights):
    first, walk, other = weights
    sds = jax.ShapeDtypeStruct
    fixed = lambda *shape: pl.BlockSpec(shape, lambda b: (0,) * len(shape))
    return pl.pallas_call(
        owner_kernel,
        grid=(1,),
        in_specs=[fixed(NP, CA + 8, D), fixed(CX + 8, D), fixed(CX + 8, D), fixed(ML, D)] + weight_specs(3),
        out_specs=(fixed(NP, CA, D), fixed(CX, D), fixed(CX, D), fixed(8, OS), fixed(8, 128)),
        out_shape=(
            sds((NP, CA, D), BF), sds((CX, D), BF), sds((CX, D), BF), sds((8, OS), F32), sds((8, 128), F32),
        ),
        scratch_shapes=[pltpu.VMEM((OS, D), BF), pltpu.VMEM((OS, 8), F32)],
        compiler_params=pltpu.CompilerParams(vmem_limit_bytes=VMEM),
        name="owner",
    )(ra, rp, rm, proj, walk, other, first)


def nodes_kernel(
    where_ref, oa_ref, op_ref, om_ref, own_msg_ref, l_ref, own_l_ref, mesh_ref,
    wi_ref, wi2_ref, wm_ref, wm2_ref, wo_ref, wo2_ref, v_ref,
    out_ref, out_s,
):
    bias = vectors_of(v_ref, 0, walk_of(where_ref[0]))[1:2]
    vec = bias + vectors_of(v_ref, 2)[1:2] + vectors_of(v_ref, 3)
    w_in, w_msg, w_out = full((wi_ref, wi2_ref)), full((wm_ref, wm2_ref)), full((wo_ref, wo2_ref))
    S = ML // 2
    for i in range(2):
        at = slice(S * i, S * i + S)
        row = (iota((S, 1), 0) + S * i).astype(F32)
        summed = dot(onehot(row == l_ref[0:1, 0:OP]), oa_ref[...].reshape(OP, D))
        summed += dot(onehot(row == l_ref[0:1, OP : OP + CX]), op_ref[...])
        summed += dot(onehot(row == l_ref[0:1, OM : OM + CX]), om_ref[...])
        summed += dot(onehot(row == own_l_ref[0:1, :]), own_msg_ref[...])
        own = mesh_ref[at, :]
        before = dot_nt(own, w_in) + dot_nt(summed.astype(BF), w_msg) + vec[0]
        hidden = silu(before).astype(BF)
        total = dot(hidden, w_out) + vec[1]
        out_s[at, :] = own.astype(F32) + normalized(total, vec[2], vec[3])
    for t in range(ML // 128):
        for k in range(4):
            turned = out_s[128 * t : 128 * t + 128, 128 * k : 128 * k + 128].T.astype(BF)
            out_ref[2 * k, 64 * t : 64 * t + 64, :] = turned[0:64]
            out_ref[2 * k + 1, 64 * t : 64 * t + 64, :] = turned[64:128]


def nodes(where, oa, op, om, own_msg, l_row, own_l, mesh_latent, weights):
    first, walk, other = weights
    sds = jax.ShapeDtypeStruct
    fixed = lambda *shape: pl.BlockSpec(shape, lambda b, w: (0,) * len(shape))
    return pl.pallas_call(
        nodes_kernel,
        grid_spec=pltpu.PrefetchScalarGridSpec(
            num_scalar_prefetch=1,
            grid=(1,),
            in_specs=[
                fixed(NP, CA, D), fixed(CX, D), fixed(CX, D), fixed(CS, D), fixed(8, OS), fixed(8, CS),
                pl.BlockSpec((ML, D), lambda b, w: (w[0], 0)),
            ] + weight_specs(1, 2, 4),
            out_specs=fixed(NH, ML // 2, 128),
            scratch_shapes=[pltpu.VMEM((ML, D), F32)],
        ),
        out_shape=sds((NH, ML // 2, 128), BF),
        compiler_params=pltpu.CompilerParams(vmem_limit_bytes=VMEM),
        name="nodes",
    )(where, oa, op, om, own_msg, l_row, own_l, mesh_latent, walk, other, walk, other, walk, other, first)


def unpack_kernel(ma_ref, mp_ref, mm_ref, ms_ref, slot_ref, flag_ref, out_ref, msg, rows):
    for n in range(NP):
        msg[CA * n : CA * n + CA, :] = ma_ref[n]
    for ref, at in ((mp_ref, OP), (mm_ref, OM)):
        msg[at : at + CX, :] = ref[...]
        msg[at + CX : at + 256, :] = jnp.zeros((256 - CX, D), BF)
    msg[OS : OS + CS, :] = ms_ref[...]
    T = 384

    for i in range(N1 // T):
        hit = onehot(iota((T, NS), 1).astype(F32) == slot_ref[T * i : T * i + T, 0:1])
        rows[T * i : T * i + T, :] = dot(hit, msg[...])
    for k in range(NH // 2):
        at = slice(128 * k, 128 * k + 128)
        a, b = lane_join(rows[0:HALF, at], rows[HALF:N1, at])
        out_ref[2 * k, 0:HALF, :] = a.astype(BF)
        out_ref[2 * k + 1, 0:HALF, :] = b.astype(BF)
    flag = jnp.concatenate([flag_ref[...]] * (FLAG // 8), axis=0).astype(BF)
    for n in range(NH):
        out_ref[n, HALF:OUT_ROWS, :] = flag


def unpack(ma, mp, mm, ms, slots, flag):
    return pl.pallas_call(
        unpack_kernel,
        out_shape=jax.ShapeDtypeStruct((NH, OUT_ROWS, 128), BF),
        scratch_shapes=[pltpu.VMEM((NS, D), BF), pltpu.VMEM((N1, D), F32)],
        compiler_params=pltpu.CompilerParams(vmem_limit_bytes=VMEM),
        name="unpack",
    )(ma, mp, mm, ms, slots, flag)


def columns_kernel(where_ref, edge_ref, out_ref):
    odd = (where_ref[0] & 1) == 1
    low = iota((128, 128), 1) < 64
    for i in range(8):
        a = edge_ref[256 * i : 256 * i + 128, :].astype(F32)
        b = edge_ref[256 * i + 128 : 256 * i + 256, :].astype(F32)
        left, right = jnp.where(low, a, pltpu.roll(b, 64, 1)), jnp.where(low, pltpu.roll(a, 64, 1), b)
        turned = jnp.where(odd, right, left).T.astype(BF)
        out_ref[:, 256 * i : 256 * i + 128] = turned[0:64]
        out_ref[:, 256 * i + 128 : 256 * i + 256] = turned[64:128]


def columns(where, edge_latent):
    return pl.pallas_call(
        columns_kernel,
        grid_spec=pltpu.PrefetchScalarGridSpec(
            num_scalar_prefetch=1,
            grid=(4,),
            in_specs=[pl.BlockSpec((E // 4, 128), lambda b, w: (b, w[0] // 2))],
            out_specs=pl.BlockSpec((64, E // 4), lambda b, w: (0, b)),
        ),
        out_shape=jax.ShapeDtypeStruct((64, E), BF),
        compiler_params=pltpu.CompilerParams(vmem_limit_bytes=VMEM),
        name="columns",
    )(where, edge_latent)


def finish_kernel(starts_ref, in_ref, mesh_in_ref, key_ref, column_ref, out_ref, mesh_ref, flag_ref, lists):
    flag = jnp.zeros((8, 128), F32)
    half = iota((HALF, 128), 1) < 64
    for n in range(NH):
        x = in_ref[n, 0:HALF, :].astype(F32)
        turned = pltpu.roll(x, 64, 1)
        lists[n, 0:HALF, :] = jnp.where(half, x, turned).astype(BF)
        lists[n, HALF:N1, :] = jnp.where(half, turned, x).astype(BF)
        lists[n, N1 : N1 + WIN, :] = jnp.zeros((WIN, 128), BF)
        flag = jnp.maximum(flag, in_ref[n, HALF : HALF + 8, :].astype(F32))
        for t in range(ML // 128):
            at = ML * n + 128 * t
            mesh_ref[:, at : at + 128] = mesh_in_ref[n, 64 * t : 64 * t + 64, :]
    flag_ref[0, 0] = (jnp.max(flag) > 0.5).astype(I32)
    low = iota((128, 128), 1) < 64
    lane = iota((128, NH * WIN), 1).astype(F32)

    def group(g, carry):
        key = key_ref[pl.ds(pl.multiple_of(8 * g, 8), 8), :]
        h = jnp.floor(key * (1.0 / 256.0))
        delta = key - 256.0 * h
        column = jnp.where((h >= 0.0) & (delta < WIN), h * WIN + delta, -1.0).T
        for i in range(4):
            sides = []
            for j in (2 * i, 2 * i + 1):
                hit = onehot(lane == column[:, j : j + 1])
                parts = []
                for n in range(NH):
                    at = jnp.minimum(starts_ref[8 * g + j, n], N1)
                    parts.append(lists[n, pl.ds(pl.multiple_of(at, 16), WIN), :])
                sides.append(dot(hit, jnp.concatenate(parts, axis=0)))
            turned = jnp.where(low, sides[0], sides[1]).T
            for k in range(2):
                at = pl.ds(pl.multiple_of(1024 * g + 256 * i + 128 * k, 128), 128)
                out_ref[:, at] = (turned[64 * k : 64 * k + 64] + column_ref[:, at].astype(F32)).astype(BF)
        return carry

    lax.fori_loop(0, 8, group, 0)


def finish(starts, lists, mesh_blocks, key, column):
    sds = jax.ShapeDtypeStruct
    smem = pl.BlockSpec(memory_space=pltpu.SMEM)
    vmem = pl.BlockSpec(memory_space=pltpu.VMEM)
    return pl.pallas_call(
        finish_kernel,
        in_specs=[smem, vmem, vmem, vmem, vmem],
        out_specs=(vmem, vmem, smem),
        out_shape=(sds((64, E), BF), sds((64, M), BF), sds((1, 1), I32)),
        scratch_shapes=[pltpu.VMEM((NH, N1 + WIN, 128), BF)],
        compiler_params=pltpu.CompilerParams(vmem_limit_bytes=VMEM),
        name="finish",
    )(starts, lists, mesh_blocks, key, column)


def exchange(a, p, m, away):
    up = [(i, (i + 1) % NP) for i in range(NP)]
    down = [(i, (i - 1) % NP) for i in range(NP)]
    first, second = (up, down) if away else (down, up)
    p = lax.ppermute(p, "patch", first)
    m = lax.ppermute(m, "patch", second)
    a = lax.all_to_all(a, "patch", split_axis=0, concat_axis=0, tiled=True)
    return a, p, m


def fast(
    grid_latent, mesh_latent, edge_latent, senders, receivers, mesh_slot, edge_counts,
    w_edge, w_sender, w_receiver, edge_bias, w_edge_out, edge_out_bias, edge_gain, edge_shift,
    w_mesh_in, w_message_in, mesh_bias, w_mesh_out, mesh_out_bias, mesh_gain, mesh_shift,
):
    patch = lax.axis_index("patch").astype(I32)
    own = lax.axis_index("hidden").astype(I32)
    where = jnp.stack([own, patch])
    vectors = (edge_bias, mesh_bias, edge_out_bias, edge_gain, edge_shift, mesh_out_bias, mesh_gain, mesh_shift)
    first, second = stacked(
        w_edge.T, w_sender.T, w_receiver.T, w_mesh_in.T, w_message_in.T, w_edge_out, w_mesh_out,
        *(v.reshape(1, 64) for v in vectors),
    )
    weights = to_all(first, second)
    key, starts, edges, sent, info, slots, slot_row = gather(
        edge_counts, where, receivers, mesh_slot, senders, edge_latent, grid_latent
    )
    sa, sp, sm, pre = pack(where, edges, sent, info, slot_row, weights[0])
    ra, rp, rm = exchange(sa, sp, sm, True)
    proj, ms, own_l = local(where, pre, slot_row, mesh_latent, weights)
    column = columns(where, edge_latent)
    oa, op, om, l_row, flag = owner(ra, rp, rm, proj, weights)
    ma, mp, mm = exchange(oa, op, om, False)
    mesh_blocks = nodes(where, oa, op, om, ms, l_row, own_l, mesh_latent, weights)
    mesh_blocks = lax.all_to_all(mesh_blocks, "hidden", split_axis=0, concat_axis=0, tiled=True)
    lists = unpack(ma, mp, mm, ms, slots, flag)
    lists = lax.all_to_all(lists, "hidden", split_axis=0, concat_axis=0, tiled=True)
    edge_out, mesh_out, flag = finish(starts, lists, mesh_blocks, key, column)
    return mesh_out.T, edge_out.T, flag


def from_everyone(x):
    copies = jnp.broadcast_to(x, (NH, *x.shape))
    return lax.all_to_all(copies, "hidden", split_axis=0, concat_axis=0, tiled=True)


def scattered(partial):
    blocks = jnp.stack(jnp.split(partial.astype(BF), NH, axis=1))
    blocks = lax.all_to_all(blocks, "hidden", split_axis=0, concat_axis=0, tiled=True)
    return blocks.astype(F32).sum(axis=0)


def split_normalized(v, gain, shift):
    total = from_everyone(jnp.stack([jnp.sum(v, axis=1), jnp.sum(v * v, axis=1)])).sum(axis=0) / D
    var = jnp.maximum(total[1] - total[0] * total[0], 0.0)
    return (v - total[0][:, None]) * lax.rsqrt(var + EPSILON)[:, None] * gain + shift


def slow(
    grid_latent, mesh_latent, edge_latent, senders, receivers, mesh_slot, edge_counts,
    w_edge, w_sender, w_receiver, edge_bias, w_edge_out, edge_out_bias, edge_gain, edge_shift,
    w_mesh_in, w_message_in, mesh_bias, w_mesh_out, mesh_out_bias, mesh_gain, mesh_shift,
):
    patch = lax.axis_index("patch").astype(I32)
    own = lax.axis_index("hidden").astype(I32)
    up = [(i, (i + 1) % NP) for i in range(NP)]
    target = jnp.take(mesh_slot, receivers)
    whose = target // M
    local = target - whose * M
    live = (jnp.arange(E, dtype=I32) < edge_counts[0]).astype(F32)
    pre = dot(edge_latent, w_edge) + jnp.take(dot(grid_latent, w_sender), senders - patch * G, axis=0) + edge_bias

    def fetch(s, state):
        block, pre = state
        here = (whose == (patch - s) % NP)[:, None]
        pre = pre + jnp.where(here, jnp.take(block, local, axis=0).astype(F32), 0.0)
        return lax.ppermute(block, "patch", up), pre

    block = dot(mesh_latent, w_receiver).astype(BF)
    _, pre = lax.fori_loop(0, NP, fetch, (block, pre))
    total = scattered(dot(silu(pre).astype(BF), w_edge_out)) + edge_out_bias
    message = split_normalized(total, edge_gain, edge_shift) * live[:, None]
    columns = lax.dynamic_slice_in_dim(edge_latent, own * 64, 64, 1)
    edge_out = (columns.astype(F32) + message).astype(BF)

    def collect(s, sums):
        here = whose == (patch - 1 - s) % NP
        part = jax.ops.segment_sum(jnp.where(here[:, None], message, 0.0), jnp.where(here, local, 0), num_segments=M)
        return lax.ppermute(sums, "patch", up) + part

    sums = lax.fori_loop(0, NP, collect, jnp.zeros((M, 64), F32))
    summed = jnp.concatenate(list(from_everyone(sums.astype(BF))), axis=1)
    before = dot(mesh_latent, w_mesh_in) + dot(summed, w_message_in) + mesh_bias
    total = scattered(dot(silu(before).astype(BF), w_mesh_out)) + mesh_out_bias
    columns = lax.dynamic_slice_in_dim(mesh_latent, own * 64, 64, 1)
    mesh_out = (columns.astype(F32) + split_normalized(total, mesh_gain, mesh_shift)).astype(BF)
    return mesh_out, edge_out


def shards(*args):
    mesh_out, edge_out, flag = fast(*args)
    return lax.cond(flag[0, 0] > 0, lambda a, done: slow(*a), lambda a, done: done, args, (mesh_out, edge_out))


def solution(mesh):
    rows, columns, units = P("patch", None), P(None, "hidden"), P("hidden")
    return jax.shard_map(
        shards,
        mesh=mesh,
        in_specs=(
            rows, rows, rows, P("patch"), P("patch"), P(), P("patch"),
            columns, columns, columns, units, P("hidden", None), units, units, units,
            columns, columns, units, P("hidden", None), units, units, units,
        ),
        out_specs=(P("patch", "hidden"), P("patch", "hidden")),
        check_vma=False,
    )
```

```python
import jax
import jax.numpy as jnp
from jax import lax
from jax.experimental import pallas as pl
from jax.experimental.pallas import tpu as pltpu
from jax.sharding import PartitionSpec as P


EPSILON = 1e-05
LANES = 128
BF = jnp.bfloat16
F32 = jnp.float32
I32 = jnp.int32

NP = 16
NH = 8
D = 512
E = 8192
G = 3072
M = 5120
ML = M // NH
ROWS = E // LANES
N1 = 1152
HALF = N1 // 2
CA = 64
CX = 160
CS = 384
FLAG = 16
MESH_AT = HALF + FLAG
OUT_ROWS = MESH_AT + ML // 2
OP = NP * CA
OM = OP + 256
OS = OM + 256
NS = OS + CS
WIN = 64
VROW = 128
WROWS = VROW + 8
STEP = 128
VMEM = 60 * 1024 * 1024


def dot(a, b):
    return jnp.dot(a, b, preferred_element_type=F32)


def dot_nt(a, b):
    return lax.dot_general(a, b, (((1,), (1,)), ((), ())), preferred_element_type=F32)


def iota(shape, axis):
    return lax.broadcasted_iota(I32, shape, axis)


def onehot(cond):
    return jnp.where(cond, 1.0, 0.0).astype(BF)


def lane_join(a, b):
    low = iota(a.shape, 1) < 64
    return jnp.where(low, a, pltpu.roll(b, 64, 1)), jnp.where(low, pltpu.roll(a, 64, 1), b)


def silu(v):
    return v / (1.0 + jnp.exp(-v))


def normalized(v, gain, shift):
    mean = jnp.mean(v, axis=1, keepdims=True)
    c = v - mean
    var = jnp.mean(c * c, axis=1, keepdims=True)
    return c * lax.rsqrt(var + EPSILON) * gain + shift


def row_of(x):
    return jnp.concatenate([x[i : i + 1, :] for i in range(x.shape[0])], axis=1)


def gather_kernel(
    count_ref, where_ref, recv_ref, slots_ref, send_ref, edge_hbm, grid_hbm,
    key_ref, starts_ref, list_ref, sent_ref, info_ref, slot_ref, slot_row_ref, tgt,
    table, hits, known, starts, edge, grid, acc, meta, edge_sem, grid_sem, starts_sem,
):
    chunk = lambda i: pltpu.make_async_copy(
        edge_hbm.at[pl.ds(i * 1024, 1024)], edge.at[pl.ds(i * 1024, 1024)], edge_sem.at[i]
    )
    for i in range(8):
        chunk(i).start()
    grid_copy = pltpu.make_async_copy(grid_hbm, grid, grid_sem)
    grid_copy.start()
    own = where_ref[0]
    patch = where_ref[1]
    v = slots_ref[...]
    table[:, 0:128] = ((v >> 8) - 160).astype(F32).astype(BF)
    table[:, 128:256] = (v & 255).astype(F32).astype(BF)

    def group(g, carry):
        r = recv_ref[pl.ds(pl.multiple_of(g * 8, 8), 8), :]
        hi = (r >> 7).astype(F32).T
        lo = (r & 127).astype(F32).T
        rows = iota((128, 640), 1).astype(F32)
        for j in range(8):
            hits[128 * j : 128 * j + 128, :] = onehot(rows == hi[:, j : j + 1])
        y = dot(hits[...], table[...])
        full = (y[:, 0:128] + 160.0) * 256.0 + y[:, 128:256]
        lane = iota((128, 128), 1).astype(F32)
        which = iota((128, 8), 1)
        got = jnp.zeros((128, 8), F32)
        for j in range(8):
            part = jnp.where(lane == lo[:, j : j + 1], full[128 * j : 128 * j + 128], 0.0)
            got = jnp.where(which == j, jnp.sum(part, axis=1, keepdims=True), got)
        tgt[pl.ds(pl.multiple_of(g * 8, 8), 8), :] = got.T
        return carry

    lax.fori_loop(0, ROWS // 8, group, 0)
    t = tgt[...]
    block = jnp.floor((t + 0.5) * (1.0 / ML))
    l = t - block * ML
    q = jnp.floor((block + 0.5) * (1.0 / NH))
    h = block - q * NH
    position = iota((ROWS, 128), 0) * 128 + iota((ROWS, 128), 1)
    live = position < count_ref[0]
    upper = onehot(iota((128, 128), 0) < iota((128, 128), 1))
    big = NH * ROWS
    row, col = iota((big, big), 0), iota((big, big), 1)
    lower = onehot((col < row) & ((col >> 6) == (row >> 6)))
    mine = [live & (h == float(k)) for k in range(NH)]
    mask = jnp.concatenate([onehot(m) for m in mine], axis=0)
    before_all = dot(mask, upper)
    counts_all = dot(mask, jnp.ones((128, 128), BF))
    above_all = dot(lower, counts_all.astype(BF))
    c = jnp.full((ROWS, 128), -1.0, F32)
    delta = jnp.full((ROWS, 128), -1.0, F32)
    begin = jnp.zeros((ROWS, 128), F32)
    totals = jnp.zeros((8, 128), F32)
    lane64 = iota((ROWS, 128), 1)
    lane8 = iota((8, 128), 1)
    for k in range(NH):
        at = slice(ROWS * k, ROWS * k + ROWS)
        above = above_all[at]
        place = before_all[at] + above
        start = jnp.floor(above * (1.0 / 16.0)) * 16.0
        c = jnp.where(mine[k], place, c)
        delta = jnp.where(mine[k], place - start, delta)
        begin = jnp.where(lane64 == k, start, begin)
        total = above[ROWS - 1 : ROWS, :] + counts_all[at][ROWS - 1 : ROWS, :]
        totals = jnp.where(lane8 == k, total, totals)
    key_ref[...] = jnp.where(delta >= 0.0, h * 256.0 + delta, -1.0)
    starts_ref[0:ROWS, :] = begin.astype(I32)
    spread = jnp.where(jnp.max(delta) >= WIN, 1.0, 0.0)
    starts_ref[ROWS : ROWS + 8, :] = totals.astype(I32)
    to_scalars = pltpu.make_async_copy(starts_ref, starts, starts_sem)
    to_scalars.start()
    acc[...] = jnp.zeros_like(acc)
    meta[...] = jnp.zeros_like(meta)
    s = (send_ref[...] - patch * G).astype(F32)
    s_hi = jnp.floor(s * (1.0 / 256.0))
    l_hi = jnp.floor(l * (1.0 / 256.0))
    kinds = [s_hi, s - 256.0 * s_hi, q, l_hi, l - 256.0 * l_hi, jnp.ones((ROWS, 128), F32)]
    kinds.append(jnp.where(h == own.astype(F32), c, -1.0))
    for k, x in enumerate(kinds):
        known[k] = x
    to_scalars.wait()
    total = starts[ROWS, own]

    def compact(i, carry):
        @pl.when(i % 2 == 0)
        def _():
            chunk(i // 2).wait()

        parts = [known[k, pl.ds(pl.multiple_of(8 * (i // 2), 8), 8), :] for k in range(7)]
        odd = i % 2 == 1
        parts = [jnp.where(odd, x[4:8], x[0:4]) for x in parts]
        c_row = row_of(parts[6])
        facts = jnp.concatenate([row_of(x) for x in parts[:6]] + [jnp.zeros((2, 512), F32)], axis=0).astype(BF)
        source = pl.ds(pl.multiple_of(512 * i, 512), 512)
        first = starts[4 * i, own]
        last = jnp.where(i == 15, total, starts[jnp.minimum(4 * i + 4, ROWS - 1), own] + 16)
        rounds = (jnp.minimum(last, N1) - first + STEP - 1) // STEP

        def add(k, carry):
            at = pl.multiple_of(first + STEP * k, 16)
            hit = onehot(c_row == (iota((STEP, 512), 0) + at).astype(F32))
            acc[pl.ds(at, STEP), :] += dot(hit, edge[source, :])
            meta[pl.ds(at, STEP), :] += dot_nt(hit, facts)
            return carry

        lax.fori_loop(0, rounds, add, 0)
        return carry

    lax.fori_loop(0, 16, compact, 0)
    grid_copy.wait()
    T = 384
    lower = onehot(iota((T, T), 1) < iota((T, T), 0))

    def place(i, state):
        carry, bad = state
        at = pl.ds(pl.multiple_of(T * i, T), T)
        facts = meta[at, :]
        valid = facts[:, 5:6] > 0.5
        sender = jnp.where(valid, facts[:, 0:1] * 256.0 + facts[:, 1:2], -1.0)
        hit = onehot(iota((T, G), 1).astype(F32) == sender)
        sent_ref[at, :] = dot(hit, grid[...]).astype(BF)
        list_ref[at, :] = acc[at, :].astype(BF)
        lane = iota((T, 128), 1)
        info = jnp.where(lane == 0, facts[:, 3:4], jnp.where(lane == 1, facts[:, 4:5], 0.0))
        info_ref[at, :] = jnp.where(lane == 2, 1.0, info).astype(BF)
        owner = jnp.where((lane.astype(F32) == facts[:, 2:3]) & valid, 1.0, 0.0)
        rank = jnp.sum(owner * (dot(lower, owner.astype(BF)) + carry), axis=1, keepdims=True)
        carry = carry + jnp.sum(owner, axis=0, keepdims=True)
        d = facts[:, 2:3] - patch.astype(F32)
        d = jnp.where(d < 0.0, d + NP, d)
        more = rank - CA
        slot = jnp.where((d == 1.0) & (more < CX), OP + more, -1.0)
        slot = jnp.where((d == NP - 1.0) & (more < CX), OM + more, slot)
        slot = jnp.where(rank < CA, facts[:, 2:3] * CA + rank, slot)
        slot = jnp.where(d == 0.0, jnp.where(rank < CS, OS + rank, -1.0), slot)
        bad = jnp.maximum(bad, jnp.max(jnp.where(valid & (slot < 0.0), 1.0, 0.0)))
        slots = jnp.broadcast_to(jnp.where(valid, slot, -1.0), (T, 128))
        slot_ref[at, :] = slots[:, 0:8]
        slot_row_ref[:, at] = slots.T[0:8, :]
        return carry, bad

    bad = jnp.maximum(jnp.where(total > N1, 1.0, 0.0), spread)
    _, bad = lax.fori_loop(0, N1 // T, place, (jnp.zeros((1, 128), F32), bad))
    slot_row_ref[:, N1 : N1 + 128] = jnp.broadcast_to(bad, (8, 128))


def gather(count, where, receivers, mesh_slot, senders, edge_latent, grid_latent):
    sds = jax.ShapeDtypeStruct
    smem = pl.BlockSpec(memory_space=pltpu.SMEM)
    vmem = pl.BlockSpec(memory_space=pltpu.VMEM)
    hbm = pl.BlockSpec(memory_space=pl.ANY)
    return pl.pallas_call(
        gather_kernel,
        out_shape=(
            sds((ROWS, 128), F32), sds((ROWS + 8, 128), I32),
            sds((N1, D), BF), sds((N1, D), BF), sds((N1, 128), BF), sds((N1, 8), F32), sds((8, N1 + 128), F32),
            sds((ROWS, 128), F32),
        ),
        in_specs=[smem, smem, vmem, vmem, vmem, hbm, hbm],
        scratch_shapes=[
            pltpu.VMEM((640, 256), BF),
            pltpu.VMEM((1024, 640), BF),
            pltpu.VMEM((7, ROWS, 128), F32),
            pltpu.SMEM((ROWS + 8, 128), I32),
            pltpu.VMEM((E, D), BF),
            pltpu.VMEM((G, D), BF),
            pltpu.VMEM((N1 + STEP, D), F32),
            pltpu.VMEM((N1 + STEP, 8), F32),
            pltpu.SemaphoreType.DMA((8,)),
            pltpu.SemaphoreType.DMA(()),
            pltpu.SemaphoreType.DMA(()),
        ],
        compiler_params=pltpu.CompilerParams(vmem_limit_bytes=VMEM),
        name="gather",
    )(
        count, where, receivers.reshape(ROWS, 128), mesh_slot.reshape(640, 128), senders.reshape(ROWS, 128),
        edge_latent, grid_latent,
    )


def walk_of(own):
    x, core = own // 2, own % 2
    places = [2 * ((x + 4 - k) % 4) for k in range(4)]
    return [p + core for p in places] + [p + 1 - core for p in places]


def vectors_of(v_ref, m, order=tuple(range(NH))):
    pairs = []
    for k in range(NH // 2):
        at = slice(128 * m, 128 * m + 128)
        x, y = v_ref[order[2 * k], :, at].astype(F32), v_ref[order[2 * k + 1], :, at].astype(F32)
        pairs.append(lane_join(x, y))
    rows = [jnp.concatenate([p[i] for p in pairs], axis=1) for i in range(2)]
    return [r[0:1] + r[1:2] + r[2:3] for r in rows]


def stack_kernel(e, s, r, mi, mm, eo, mo, *refs):
    vectors, (first_ref, second_ref) = refs[:8], refs[8:]
    for k, w in enumerate((r, mi, mm, eo, mo)):
        second_ref[64 * k : 64 * k + 64, :] = w[...]
    v = jnp.concatenate([x[...] for x in vectors], axis=1)
    v = jnp.broadcast_to(v, (8, D))
    hi = v.astype(BF)
    v = v - hi.astype(F32)
    mid = v.astype(BF)
    low = (v - mid.astype(F32)).astype(BF)
    row = iota((8, D), 0)
    parts = jnp.where(row == 0, hi.astype(F32), jnp.where(row == 1, mid.astype(F32), low.astype(F32)))
    parts = jnp.where(row < 3, parts, 0.0).astype(BF)
    for n in range(NH):
        first_ref[n, 0:64, :] = e[...]
        first_ref[n, 64:128, :] = s[...]
        first_ref[n, VROW:WROWS, :] = parts


def stacked(*args):
    return pl.pallas_call(
        stack_kernel,
        out_shape=(jax.ShapeDtypeStruct((NH, WROWS, D), BF), jax.ShapeDtypeStruct((320, D), BF)),
        name="stacked",
    )(*args)


def to_all(first, second):
    first = lax.all_to_all(first, "hidden", split_axis=0, concat_axis=0, tiled=True)
    walk = [second]
    for k in (1, 2, 3):
        walk.append(lax.ppermute(second, "hidden", [(i, (i + 2 * k) % NH) for i in range(NH)]))
    walk = jnp.stack(walk)
    other = lax.ppermute(walk, "hidden", [(i, i ^ 1) for i in range(NH)])
    return first, walk, other


def pack_kernel(where_ref, list_ref, sent_ref, info_ref, slot_row_ref, first_ref, oa_ref, op_ref, om_ref, pre, wide):
    order = walk_of(where_ref[0])
    w_edge = jnp.concatenate([first_ref[n, 0:64, :] for n in order], axis=0)
    w_sender = jnp.concatenate([first_ref[n, 64:128, :] for n in order], axis=0)
    bias = vectors_of(first_ref.at[:, VROW:WROWS], 0, order)[0]
    T = 384

    def first_layer(i, carry):
        at = pl.ds(pl.multiple_of(T * i, T), T)
        pre[at, 0:D] = (dot_nt(list_ref[at, :], w_edge) + dot_nt(sent_ref[at, :], w_sender) + bias).astype(BF)
        return carry

    lax.fori_loop(0, N1 // T, first_layer, 0)
    pre[:, D : D + 128] = info_ref[...]

    def spread(i, carry):
        hit = onehot((iota((T, N1), 0) + T * i).astype(F32) == slot_row_ref[0:1, 0:N1])
        wide[pl.ds(pl.multiple_of(T * i, T), T), :] = dot(hit, pre[...])
        return carry

    lax.fori_loop(0, OS // T, spread, 0)
    kind = iota((8, 128), 0)
    bad = slot_row_ref[0:8, N1 : N1 + 128]

    def facts_of(at):
        return jnp.where(kind == 3, bad, wide[at : at + 128, D : D + 128].T[0:8, :])

    for i in range(NP // 2):
        x = facts_of(128 * i)
        low = iota((8, 128), 1) < 64
        turned = pltpu.roll(x, 64, 1)
        for odd in range(2):
            n = 2 * i + odd
            oa_ref[n, 0:CA, :] = wide[CA * n : CA * n + CA, 0:D].astype(BF)
            both = jnp.where(low, turned, x) if odd else jnp.where(low, x, turned)
            oa_ref[n, CA : CA + 8, :] = jnp.zeros((8, D), BF)
            oa_ref[n, CA : CA + 8, 0:128] = both.astype(BF)
    for ref, at, size in ((op_ref, OP, CX), (om_ref, OM, CX)):
        ref[0:size, :] = wide[at : at + size, 0:D].astype(BF)
        ref[size : size + 8, :] = jnp.zeros((8, D), BF)
        for k in range((size + 127) // 128):
            ref[size : size + 8, 128 * k : 128 * k + 128] = facts_of(at + 128 * k).astype(BF)


def pack(where, edges, sent, info, slot_row, first):
    sds = jax.ShapeDtypeStruct
    fixed = lambda *shape: pl.BlockSpec(shape, lambda b: (0,) * len(shape))
    shapes = ((NP, CA + 8, D), (CX + 8, D), (CX + 8, D), (N1, D + 128))
    return pl.pallas_call(
        pack_kernel,
        grid=(1,),
        in_specs=[pl.BlockSpec(memory_space=pltpu.SMEM)]
        + [fixed(N1, D), fixed(N1, D), fixed(N1, 128), fixed(8, N1 + 128), fixed(NH, WROWS, D)],
        out_specs=tuple(fixed(*x) for x in shapes),
        out_shape=tuple(sds(x, BF) for x in shapes),
        scratch_shapes=[pltpu.VMEM((OS, D + 128), F32)],
        compiler_params=pltpu.CompilerParams(vmem_limit_bytes=VMEM),
        name="pack",
    )(where, edges, sent, info, slot_row, first)


def full(w_refs):
    return jnp.concatenate([w[...].reshape(D // 2, D) for w in w_refs], axis=0)


def weight_specs(*which):
    one = lambda k: pl.BlockSpec((NH // 2, 64, D), lambda *_: (0, k, 0))
    vec = pl.BlockSpec((NH, 8, D), lambda *_: (0, VROW // 8, 0))
    return [one(k) for k in which for _ in range(2)] + [vec]


def messages(x, l, proj, w_out, vec):
    hit = onehot(iota((x.shape[0], ML), 1).astype(F32) == l)
    hidden = silu(x + dot(hit, proj)).astype(BF)
    message = normalized(dot(hidden, w_out) + vec[0], vec[1], vec[2])
    return jnp.where(l >= 0.0, message, 0.0).astype(BF)


def edge_vectors(v_ref):
    return vectors_of(v_ref, 1) + vectors_of(v_ref, 2)[0:1]


def local_kernel(where_ref, pre_ref, slot_row_ref, mesh_ref, wr_ref, wr2_ref, wo_ref, wo2_ref, v_ref, proj_ref, msg_ref, l_ref):
    proj = dot_nt(mesh_ref[...], full((wr_ref, wr2_ref))).astype(BF)
    proj_ref[...] = proj
    vec = edge_vectors(v_ref)
    w_out = full((wo_ref, wo2_ref))
    T = 128

    def some(i, carry):
        at = pl.ds(pl.multiple_of(T * i, T), T)
        hit = onehot((iota((T, N1), 0) + OS + T * i).astype(F32) == slot_row_ref[0:1, 0:N1])
        x = dot(hit, pre_ref[...])
        l = jnp.where(x[:, D + 2 : D + 3] > 0.5, x[:, D : D + 1] * 256.0 + x[:, D + 1 : D + 2], -1.0)
        msg_ref[at, :] = messages(x[:, 0:D], l, proj_ref[...], w_out, vec)
        l_ref[:, at] = jnp.broadcast_to(l, (T, 128)).T[0:8, :]
        return carry

    lax.fori_loop(0, CS // T, some, 0)


def local(where, pre, slot_row, mesh_latent, weights):
    first, walk, other = weights
    sds = jax.ShapeDtypeStruct
    fixed = lambda *shape: pl.BlockSpec(shape, lambda b, w: (0,) * len(shape))
    return pl.pallas_call(
        local_kernel,
        grid_spec=pltpu.PrefetchScalarGridSpec(
            num_scalar_prefetch=1,
            grid=(1,),
            in_specs=[
                fixed(N1, D + 128), fixed(8, N1 + 128),
                pl.BlockSpec((ML, D), lambda b, w: (w[0], 0)),
            ] + weight_specs(0, 3),
            out_specs=(fixed(ML, D), fixed(CS, D), fixed(8, CS)),
        ),
        out_shape=(sds((ML, D), BF), sds((CS, D), BF), sds((8, CS), F32)),
        compiler_params=pltpu.CompilerParams(vmem_limit_bytes=VMEM),
        name="local",
    )(where, pre, slot_row, mesh_latent, walk, other, walk, other, first)


def owner_kernel(
    ra_ref, rp_ref, rm_ref, proj_ref, wo_ref, wo2_ref, v_ref,
    oa_ref, op_ref, om_ref, l_row_ref, flag_ref,
    x_s, l_col,
):
    low = iota((8, 128), 1) < 64
    flags = jnp.zeros((8, 128), F32)
    pieces = []
    for i in range(NP // 2):
        a = ra_ref[2 * i, CA : CA + 8, 0:128].astype(F32)
        b = ra_ref[2 * i + 1, CA : CA + 8, 0:128].astype(F32)
        pieces.append(jnp.where(low, a, b))
    for ref, size in ((rp_ref, CX), (rm_ref, CX)):
        for k in range((size + 127) // 128):
            pieces.append(ref[size : size + 8, 128 * k : 128 * k + 128].astype(F32))
    for k, m in enumerate(pieces):
        flags = jnp.maximum(flags, m)
        l = jnp.where(m[2:3] > 0.5, m[0:1] * 256.0 + m[1:2], -1.0)
        l = jnp.broadcast_to(l, (8, 128))
        l_row_ref[:, 128 * k : 128 * k + 128] = l
        l_col[128 * k : 128 * k + 128, :] = l.T
    flag_ref[...] = jnp.broadcast_to(flags[3:4], (8, 128))
    for n in range(NP):
        x_s[CA * n : CA * n + CA, :] = ra_ref[n, 0:CA, :]
    for ref, at in ((rp_ref, OP), (rm_ref, OM)):
        x_s[at : at + CX, :] = ref[0:CX, :]
        x_s[at + CX : at + 256, :] = jnp.zeros((256 - CX, D), BF)
    vec = edge_vectors(v_ref)
    w_out = full((wo_ref, wo2_ref))
    T = 384

    def some(i, carry):
        at = pl.ds(pl.multiple_of(T * i, T), T)
        x_s[at, :] = messages(x_s[at, :].astype(F32), l_col[at, 0:1], proj_ref[...], w_out, vec)
        return carry

    lax.fori_loop(0, OS // T, some, 0)
    for n in range(NP):
        oa_ref[n, :, :] = x_s[CA * n : CA * n + CA, :]
    op_ref[...] = x_s[OP : OP + CX, :]
    om_ref[...] = x_s[OM : OM + CX, :]


def owner(ra, rp, rm, proj, weights):
    first, walk, other = weights
    sds = jax.ShapeDtypeStruct
    fixed = lambda *shape: pl.BlockSpec(shape, lambda b: (0,) * len(shape))
    return pl.pallas_call(
        owner_kernel,
        grid=(1,),
        in_specs=[fixed(NP, CA + 8, D), fixed(CX + 8, D), fixed(CX + 8, D), fixed(ML, D)] + weight_specs(3),
        out_specs=(fixed(NP, CA, D), fixed(CX, D), fixed(CX, D), fixed(8, OS), fixed(8, 128)),
        out_shape=(
            sds((NP, CA, D), BF), sds((CX, D), BF), sds((CX, D), BF), sds((8, OS), F32), sds((8, 128), F32),
        ),
        scratch_shapes=[pltpu.VMEM((OS, D), BF), pltpu.VMEM((OS, 8), F32)],
        compiler_params=pltpu.CompilerParams(vmem_limit_bytes=VMEM),
        name="owner",
    )(ra, rp, rm, proj, walk, other, first)


def nodes_kernel(
    where_ref, oa_ref, op_ref, om_ref, own_msg_ref, l_ref, own_l_ref, mesh_ref,
    wi_ref, wi2_ref, wm_ref, wm2_ref, wo_ref, wo2_ref, v_ref,
    out_ref, out_s,
):
    bias = vectors_of(v_ref, 0, walk_of(where_ref[0]))[1:2]
    vec = bias + vectors_of(v_ref, 2)[1:2] + vectors_of(v_ref, 3)
    w_in, w_msg, w_out = full((wi_ref, wi2_ref)), full((wm_ref, wm2_ref)), full((wo_ref, wo2_ref))
    S = ML // 4

    def some(i, carry):
        at = pl.ds(pl.multiple_of(S * i, S), S)
        row = (iota((S, 1), 0) + S * i).astype(F32)
        summed = dot(onehot(row == l_ref[0:1, 0:OP]), oa_ref[...].reshape(OP, D))
        summed += dot(onehot(row == l_ref[0:1, OP : OP + CX]), op_ref[...])
        summed += dot(onehot(row == l_ref[0:1, OM : OM + CX]), om_ref[...])
        summed += dot(onehot(row == own_l_ref[0:1, :]), own_msg_ref[...])
        own = mesh_ref[at, :]
        before = dot_nt(own, w_in) + dot_nt(summed.astype(BF), w_msg) + vec[0]
        hidden = silu(before).astype(BF)
        total = dot(hidden, w_out) + vec[1]
        out_s[at, :] = own.astype(F32) + normalized(total, vec[2], vec[3])
        return carry

    lax.fori_loop(0, 4, some, 0)
    for t in range(ML // 128):
        for k in range(4):
            turned = out_s[128 * t : 128 * t + 128, 128 * k : 128 * k + 128].T.astype(BF)
            out_ref[2 * k, 64 * t : 64 * t + 64, :] = turned[0:64]
            out_ref[2 * k + 1, 64 * t : 64 * t + 64, :] = turned[64:128]


def nodes(where, oa, op, om, own_msg, l_row, own_l, mesh_latent, weights):
    first, walk, other = weights
    sds = jax.ShapeDtypeStruct
    fixed = lambda *shape: pl.BlockSpec(shape, lambda b, w: (0,) * len(shape))
    return pl.pallas_call(
        nodes_kernel,
        grid_spec=pltpu.PrefetchScalarGridSpec(
            num_scalar_prefetch=1,
            grid=(1,),
            in_specs=[
                fixed(NP, CA, D), fixed(CX, D), fixed(CX, D), fixed(CS, D), fixed(8, OS), fixed(8, CS),
                pl.BlockSpec((ML, D), lambda b, w: (w[0], 0)),
            ] + weight_specs(1, 2, 4),
            out_specs=fixed(NH, ML // 2, 128),
            scratch_shapes=[pltpu.VMEM((ML, D), F32)],
        ),
        out_shape=sds((NH, ML // 2, 128), BF),
        compiler_params=pltpu.CompilerParams(vmem_limit_bytes=VMEM),
        name="nodes",
    )(where, oa, op, om, own_msg, l_row, own_l, mesh_latent, walk, other, walk, other, walk, other, first)


def unpack_kernel(ma_ref, mp_ref, mm_ref, ms_ref, slot_ref, flag_ref, mesh_ref, out_ref, msg, rows):
    for n in range(NP):
        msg[CA * n : CA * n + CA, :] = ma_ref[n]
    for ref, at in ((mp_ref, OP), (mm_ref, OM)):
        msg[at : at + CX, :] = ref[...]
        msg[at + CX : at + 256, :] = jnp.zeros((256 - CX, D), BF)
    msg[OS : OS + CS, :] = ms_ref[...]
    T = 384

    def one(i, carry):
        at = pl.ds(pl.multiple_of(T * i, T), T)
        hit = onehot(iota((T, NS), 1).astype(F32) == slot_ref[at, 0:1])
        rows[at, :] = dot(hit, msg[...])
        return carry

    lax.fori_loop(0, N1 // T, one, 0)
    for k in range(NH // 2):
        at = slice(128 * k, 128 * k + 128)
        a, b = lane_join(rows[0:HALF, at], rows[HALF:N1, at])
        out_ref[2 * k, 0:HALF, :] = a.astype(BF)
        out_ref[2 * k + 1, 0:HALF, :] = b.astype(BF)
    flag = jnp.concatenate([flag_ref[...]] * (FLAG // 8), axis=0).astype(BF)
    for n in range(NH):
        out_ref[n, HALF:MESH_AT, :] = flag
        out_ref[n, MESH_AT:OUT_ROWS, :] = mesh_ref[n]


def unpack(ma, mp, mm, ms, slots, flag, mesh_blocks):
    return pl.pallas_call(
        unpack_kernel,
        out_shape=jax.ShapeDtypeStruct((NH, OUT_ROWS, 128), BF),
        scratch_shapes=[pltpu.VMEM((NS, D), BF), pltpu.VMEM((N1, D), F32)],
        compiler_params=pltpu.CompilerParams(vmem_limit_bytes=VMEM),
        name="unpack",
    )(ma, mp, mm, ms, slots, flag, mesh_blocks)


def columns_kernel(where_ref, edge_ref, out_ref):
    odd = (where_ref[0] & 1) == 1
    low = iota((128, 128), 1) < 64
    for i in range(8):
        a = edge_ref[256 * i : 256 * i + 128, :].astype(F32)
        b = edge_ref[256 * i + 128 : 256 * i + 256, :].astype(F32)
        left, right = jnp.where(low, a, pltpu.roll(b, 64, 1)), jnp.where(low, pltpu.roll(a, 64, 1), b)
        turned = jnp.where(odd, right, left).T.astype(BF)
        out_ref[:, 256 * i : 256 * i + 128] = turned[0:64]
        out_ref[:, 256 * i + 128 : 256 * i + 256] = turned[64:128]


def columns(where, edge_latent):
    return pl.pallas_call(
        columns_kernel,
        grid_spec=pltpu.PrefetchScalarGridSpec(
            num_scalar_prefetch=1,
            grid=(4,),
            in_specs=[pl.BlockSpec((E // 4, 128), lambda b, w: (b, w[0] // 2))],
            out_specs=pl.BlockSpec((64, E // 4), lambda b, w: (0, b)),
        ),
        out_shape=jax.ShapeDtypeStruct((64, E), BF),
        compiler_params=pltpu.CompilerParams(vmem_limit_bytes=VMEM),
        name="columns",
    )(where, edge_latent)


def finish_kernel(starts_ref, in_ref, key_ref, column_ref, out_ref, mesh_ref, flag_ref, lists):
    flag = jnp.zeros((8, 128), F32)
    half = iota((HALF, 128), 1) < 64
    for n in range(NH):
        x = in_ref[n, 0:HALF, :].astype(F32)
        turned = pltpu.roll(x, 64, 1)
        lists[n, 0:HALF, :] = jnp.where(half, x, turned).astype(BF)
        lists[n, HALF:N1, :] = jnp.where(half, turned, x).astype(BF)
        lists[n, N1 : N1 + WIN, :] = jnp.zeros((WIN, 128), BF)
        flag = jnp.maximum(flag, in_ref[n, HALF : HALF + 8, :].astype(F32))
        for t in range(ML // 128):
            at = ML * n + 128 * t
            mesh_ref[:, at : at + 128] = in_ref[n, MESH_AT + 64 * t : MESH_AT + 64 * t + 64, :]
    flag_ref[0, 0] = (jnp.max(flag) > 0.5).astype(I32)
    low = iota((128, 128), 1) < 64
    lane = iota((128, NH * WIN), 1).astype(F32)

    def group(g, carry):
        key = key_ref[pl.ds(pl.multiple_of(8 * g, 8), 8), :]
        h = jnp.floor(key * (1.0 / 256.0))
        delta = key - 256.0 * h
        column = jnp.where((h >= 0.0) & (delta < WIN), h * WIN + delta, -1.0).T
        for i in range(4):
            sides = []
            for j in (2 * i, 2 * i + 1):
                hit = onehot(lane == column[:, j : j + 1])
                parts = []
                for n in range(NH):
                    at = jnp.minimum(starts_ref[8 * g + j, n], N1)
                    parts.append(lists[n, pl.ds(pl.multiple_of(at, 16), WIN), :])
                sides.append(dot(hit, jnp.concatenate(parts, axis=0)))
            turned = jnp.where(low, sides[0], sides[1]).T
            for k in range(2):
                at = pl.ds(pl.multiple_of(1024 * g + 256 * i + 128 * k, 128), 128)
                out_ref[:, at] = (turned[64 * k : 64 * k + 64] + column_ref[:, at].astype(F32)).astype(BF)
        return carry

    lax.fori_loop(0, 8, group, 0)


def finish(starts, lists, key, column):
    sds = jax.ShapeDtypeStruct
    smem = pl.BlockSpec(memory_space=pltpu.SMEM)
    vmem = pl.BlockSpec(memory_space=pltpu.VMEM)
    return pl.pallas_call(
        finish_kernel,
        in_specs=[smem, vmem, vmem, vmem],
        out_specs=(vmem, vmem, smem),
        out_shape=(sds((64, E), BF), sds((64, M), BF), sds((1, 1), I32)),
        scratch_shapes=[pltpu.VMEM((NH, N1 + WIN, 128), BF)],
        compiler_params=pltpu.CompilerParams(vmem_limit_bytes=VMEM),
        name="finish",
    )(starts, lists, key, column)


def exchange(a, p, m, away):
    up = [(i, (i + 1) % NP) for i in range(NP)]
    down = [(i, (i - 1) % NP) for i in range(NP)]
    first, second = (up, down) if away else (down, up)
    p = lax.ppermute(p, "patch", first)
    m = lax.ppermute(m, "patch", second)
    a = lax.all_to_all(a, "patch", split_axis=0, concat_axis=0, tiled=True)
    return a, p, m


def fast(
    grid_latent, mesh_latent, edge_latent, senders, receivers, mesh_slot, edge_counts,
    w_edge, w_sender, w_receiver, edge_bias, w_edge_out, edge_out_bias, edge_gain, edge_shift,
    w_mesh_in, w_message_in, mesh_bias, w_mesh_out, mesh_out_bias, mesh_gain, mesh_shift,
):
    patch = lax.axis_index("patch").astype(I32)
    own = lax.axis_index("hidden").astype(I32)
    where = jnp.stack([own, patch])
    vectors = (edge_bias, mesh_bias, edge_out_bias, edge_gain, edge_shift, mesh_out_bias, mesh_gain, mesh_shift)
    first, second = stacked(
        w_edge.T, w_sender.T, w_receiver.T, w_mesh_in.T, w_message_in.T, w_edge_out, w_mesh_out,
        *(v.reshape(1, 64) for v in vectors),
    )
    weights = to_all(first, second)
    key, starts, edges, sent, info, slots, slot_row, target = gather(
        edge_counts, where, receivers, mesh_slot, senders, edge_latent, grid_latent
    )
    sa, sp, sm, pre = pack(where, edges, sent, info, slot_row, weights[0])
    ra, rp, rm = exchange(sa, sp, sm, True)
    proj, ms, own_l = local(where, pre, slot_row, mesh_latent, weights)
    column = columns(where, edge_latent)
    oa, op, om, l_row, flag = owner(ra, rp, rm, proj, weights)
    ma, mp, mm = exchange(oa, op, om, False)
    mesh_blocks = nodes(where, oa, op, om, ms, l_row, own_l, mesh_latent, weights)
    lists = unpack(ma, mp, mm, ms, slots, flag, mesh_blocks)
    lists = lax.all_to_all(lists, "hidden", split_axis=0, concat_axis=0, tiled=True)
    edge_out, mesh_out, flag = finish(starts, lists, key, column)
    return mesh_out.T, edge_out.T, flag, target


def from_everyone(x):
    copies = jnp.broadcast_to(x, (NH, *x.shape))
    return lax.all_to_all(copies, "hidden", split_axis=0, concat_axis=0, tiled=True)


def by_rows(f, size, *xs):
    part = lambda x, i: lax.dynamic_slice_in_dim(x, size * i, size)
    shape = jax.eval_shape(f, *(jax.ShapeDtypeStruct((size, *x.shape[1:]), x.dtype) for x in xs))
    out = jnp.zeros((xs[0].shape[0], *shape.shape[1:]), shape.dtype)

    def one(i, out):
        return lax.dynamic_update_slice_in_dim(out, f(*(part(x, i) for x in xs)), size * i, 0)

    return lax.fori_loop(0, xs[0].shape[0] // size, one, out)


def times(x, w):
    return by_rows(lambda y: dot(y, w), 128, x)


def rows_at(table, index):
    ids = jnp.arange(table.shape[0], dtype=I32)
    return by_rows(lambda at: dot((at[:, None] == ids[None, :]).astype(BF), table), 128, index)


def sums_at(rows, index):
    def some(ids):
        def one(i, out):
            at = lax.dynamic_slice_in_dim(index, 512 * i, 512)
            return out + dot((ids[:, None] == at[None, :]).astype(BF), lax.dynamic_slice_in_dim(rows, 512 * i, 512))

        return lax.fori_loop(0, E // 512, one, jnp.zeros((ids.shape[0], rows.shape[1]), F32))

    return by_rows(some, 128, jnp.arange(M, dtype=I32))


def second_layer(pre, w):
    partial = by_rows(lambda x: dot(silu(x).astype(BF), w).astype(BF), 128, pre)
    blocks = lax.all_to_all(jnp.stack(jnp.split(partial, NH, axis=1)), "hidden", split_axis=0, concat_axis=0, tiled=True)
    return by_rows(lambda *x: sum(y.astype(F32) for y in x), 128, *blocks)


def finished(v, gain, shift, scale, columns):
    parts = by_rows(lambda x: jnp.stack([jnp.sum(x, axis=1), jnp.sum(x * x, axis=1)], axis=1), 128, v)
    total = from_everyone(parts.T).sum(axis=0).T / D

    def one(x, t, scale):
        var = jnp.maximum(t[:, 1:2] - t[:, 0:1] * t[:, 0:1], 0.0)
        return ((x - t[:, 0:1]) * lax.rsqrt(var + EPSILON) * gain + shift) * scale

    change = by_rows(one, 128, v, total, scale)
    return by_rows(lambda c, x: (c.astype(F32) + x).astype(BF), 128, columns, change), change


def slow(
    target,
    grid_latent, mesh_latent, edge_latent, senders, receivers, mesh_slot, edge_counts,
    w_edge, w_sender, w_receiver, edge_bias, w_edge_out, edge_out_bias, edge_gain, edge_shift,
    w_mesh_in, w_message_in, mesh_bias, w_mesh_out, mesh_out_bias, mesh_gain, mesh_shift,
):
    patch = lax.axis_index("patch").astype(I32)
    own = lax.axis_index("hidden").astype(I32)
    up = [(i, (i + 1) % NP) for i in range(NP)]
    target = target.astype(I32).reshape(E)
    whose = target // M
    local = target - whose * M
    live = (jnp.arange(E, dtype=I32) < edge_counts[0]).astype(F32)
    sent = rows_at(grid_latent, senders - patch * G).astype(BF)
    pre = times(edge_latent, w_edge) + times(sent, w_sender) + edge_bias

    def fetch(s, state):
        block, pre = state
        pre = pre + rows_at(block, jnp.where(whose == (patch - s) % NP, local, -1))
        return lax.ppermute(block, "patch", up), pre

    block = times(mesh_latent, w_receiver).astype(BF)
    _, pre = lax.fori_loop(0, NP, fetch, (block, pre))
    total = second_layer(pre, w_edge_out) + edge_out_bias
    columns = lax.dynamic_slice_in_dim(edge_latent, own * 64, 64, 1)
    edge_out, message = finished(total, edge_gain, edge_shift, live[:, None], columns)
    rows = message.astype(BF)

    def collect(s, sums):
        part = sums_at(rows, jnp.where(whose == (patch - 1 - s) % NP, local, -1))
        return lax.ppermute(sums, "patch", up) + part

    sums = lax.fori_loop(0, NP, collect, jnp.zeros((M, 64), F32))
    summed = jnp.concatenate(list(from_everyone(sums.astype(BF))), axis=1)
    before = times(mesh_latent, w_mesh_in) + times(summed, w_message_in) + mesh_bias
    total = second_layer(before, w_mesh_out) + mesh_out_bias
    columns = lax.dynamic_slice_in_dim(mesh_latent, own * 64, 64, 1)
    mesh_out, _ = finished(total, mesh_gain, mesh_shift, jnp.ones((M, 1), F32), columns)
    return mesh_out, edge_out


def shards(*args):
    mesh_out, edge_out, flag, target = fast(*args)
    return lax.cond(
        flag[0, 0] > 0, lambda a, done: slow(*a), lambda a, done: done, (target, *args), (mesh_out, edge_out)
    )


def solution(mesh):
    rows, columns, units = P("patch", None), P(None, "hidden"), P("hidden")
    return jax.shard_map(
        shards,
        mesh=mesh,
        in_specs=(
            rows, rows, rows, P("patch"), P("patch"), P(), P("patch"),
            columns, columns, columns, units, P("hidden", None), units, units, units,
            columns, columns, units, P("hidden", None), units, units, units,
        ),
        out_specs=(P("patch", "hidden"), P("patch", "hidden")),
        check_vma=False,
    )
```

```python
import jax
import jax.numpy as jnp
from jax import lax
from jax.experimental import pallas as pl
from jax.experimental.pallas import tpu as pltpu
from jax.sharding import PartitionSpec as P


EPSILON = 1e-05
LANES = 128
BF = jnp.bfloat16
F32 = jnp.float32
I32 = jnp.int32

NP = 16
NH = 8
D = 512
E = 8192
G = 3072
M = 5120
ML = M // NH
ROWS = E // LANES
N1 = 1152
HALF = N1 // 2
CA = 64
CX = 160
CS = 384
FLAG = 16
MESH_AT = HALF + FLAG
OUT_ROWS = MESH_AT + ML // 2
OP = NP * CA
OM = OP + 256
OS = OM + 256
NS = OS + CS
WIN = 64
VROW = 128
WROWS = VROW + 8
STEP = 128
VMEM = 60 * 1024 * 1024


def dot(a, b):
    return jnp.dot(a, b, preferred_element_type=F32)


def dot_nt(a, b):
    return lax.dot_general(a, b, (((1,), (1,)), ((), ())), preferred_element_type=F32)


def iota(shape, axis):
    return lax.broadcasted_iota(I32, shape, axis)


def onehot(cond):
    return jnp.where(cond, 1.0, 0.0).astype(BF)


def lane_join(a, b):
    low = iota(a.shape, 1) < 64
    return jnp.where(low, a, pltpu.roll(b, 64, 1)), jnp.where(low, pltpu.roll(a, 64, 1), b)


def silu(v):
    return v / (1.0 + jnp.exp(-v))


def normalized(v, gain, shift):
    mean = jnp.mean(v, axis=1, keepdims=True)
    c = v - mean
    var = jnp.mean(c * c, axis=1, keepdims=True)
    return c * lax.rsqrt(var + EPSILON) * gain + shift


def row_of(x):
    return jnp.concatenate([x[i : i + 1, :] for i in range(x.shape[0])], axis=1)


def gather_kernel(
    count_ref, where_ref, recv_ref, slots_ref, send_ref, edge_hbm, grid_hbm,
    key_ref, starts_ref, list_ref, sent_ref, info_ref, slot_ref, slot_row_ref, tgt,
    table, hits, known, starts, edge, grid, acc, meta, edge_sem, grid_sem, starts_sem,
):
    chunk = lambda i: pltpu.make_async_copy(
        edge_hbm.at[pl.ds(i * 1024, 1024)], edge.at[pl.ds(i * 1024, 1024)], edge_sem.at[i]
    )
    for i in range(8):
        chunk(i).start()
    grid_copy = pltpu.make_async_copy(grid_hbm, grid, grid_sem)
    grid_copy.start()
    own = where_ref[0]
    patch = where_ref[1]
    v = slots_ref[...]
    table[:, 0:128] = ((v >> 8) - 160).astype(F32).astype(BF)
    table[:, 128:256] = (v & 255).astype(F32).astype(BF)

    def group(g, carry):
        r = recv_ref[pl.ds(pl.multiple_of(g * 8, 8), 8), :]
        hi = (r >> 7).astype(F32).T
        lo = (r & 127).astype(F32).T
        rows = iota((128, 640), 1).astype(F32)
        for j in range(8):
            hits[128 * j : 128 * j + 128, :] = onehot(rows == hi[:, j : j + 1])
        y = dot(hits[...], table[...])
        full = (y[:, 0:128] + 160.0) * 256.0 + y[:, 128:256]
        lane = iota((128, 128), 1).astype(F32)
        which = iota((128, 8), 1)
        got = jnp.zeros((128, 8), F32)
        for j in range(8):
            part = jnp.where(lane == lo[:, j : j + 1], full[128 * j : 128 * j + 128], 0.0)
            got = jnp.where(which == j, jnp.sum(part, axis=1, keepdims=True), got)
        tgt[pl.ds(pl.multiple_of(g * 8, 8), 8), :] = got.T
        return carry

    lax.fori_loop(0, ROWS // 8, group, 0)
    t = tgt[...]
    block = jnp.floor((t + 0.5) * (1.0 / ML))
    l = t - block * ML
    q = jnp.floor((block + 0.5) * (1.0 / NH))
    h = block - q * NH
    position = iota((ROWS, 128), 0) * 128 + iota((ROWS, 128), 1)
    live = position < count_ref[0]
    upper = onehot(iota((128, 128), 0) < iota((128, 128), 1))
    big = NH * ROWS
    row, col = iota((big, big), 0), iota((big, big), 1)
    lower = onehot((col < row) & ((col >> 6) == (row >> 6)))
    mine = [live & (h == float(k)) for k in range(NH)]
    mask = jnp.concatenate([onehot(m) for m in mine], axis=0)
    before_all = dot(mask, upper)
    counts_all = dot(mask, jnp.ones((128, 128), BF))
    above_all = dot(lower, counts_all.astype(BF))
    c = jnp.full((ROWS, 128), -1.0, F32)
    delta = jnp.full((ROWS, 128), -1.0, F32)
    begin = jnp.zeros((ROWS, 128), F32)
    totals = jnp.zeros((8, 128), F32)
    lane64 = iota((ROWS, 128), 1)
    lane8 = iota((8, 128), 1)
    for k in range(NH):
        at = slice(ROWS * k, ROWS * k + ROWS)
        above = above_all[at]
        place = before_all[at] + above
        start = jnp.floor(above * (1.0 / 16.0)) * 16.0
        c = jnp.where(mine[k], place, c)
        delta = jnp.where(mine[k], place - start, delta)
        begin = jnp.where(lane64 == k, start, begin)
        total = above[ROWS - 1 : ROWS, :] + counts_all[at][ROWS - 1 : ROWS, :]
        totals = jnp.where(lane8 == k, total, totals)
    key_ref[...] = jnp.where(delta >= 0.0, h * 256.0 + delta, -1.0)
    starts_ref[0:ROWS, :] = begin.astype(I32)
    spread = jnp.where(jnp.max(delta) >= WIN, 1.0, 0.0)
    starts_ref[ROWS : ROWS + 8, :] = totals.astype(I32)
    to_scalars = pltpu.make_async_copy(starts_ref, starts, starts_sem)
    to_scalars.start()
    acc[...] = jnp.zeros_like(acc)
    meta[...] = jnp.zeros_like(meta)
    s = (send_ref[...] - patch * G).astype(F32)
    s_hi = jnp.floor(s * (1.0 / 256.0))
    l_hi = jnp.floor(l * (1.0 / 256.0))
    kinds = [s_hi, s - 256.0 * s_hi, q, l_hi, l - 256.0 * l_hi, jnp.ones((ROWS, 128), F32)]
    kinds.append(jnp.where(h == own.astype(F32), c, -1.0))
    for k, x in enumerate(kinds):
        known[k] = x
    to_scalars.wait()
    total = starts[ROWS, own]

    def compact(i, carry):
        chunk(i).wait()
        parts = [known[k, pl.ds(pl.multiple_of(8 * i, 8), 8), :] for k in range(7)]
        for half in range(2):
            rows = slice(4 * half, 4 * half + 4)
            c_row = row_of(parts[6][rows])
            facts = [row_of(x[rows]) for x in parts[:6]] + [jnp.zeros((2, 512), F32)]
            facts = jnp.concatenate(facts, axis=0).astype(BF)
            source = pl.ds(pl.multiple_of(1024 * i + 512 * half, 512), 512)

            def add(at, c_row=c_row, facts=facts, source=source):
                hit = onehot(c_row == (iota((STEP, 512), 0) + at).astype(F32))
                acc[pl.ds(at, STEP), :] += dot(hit, edge[source, :])
                meta[pl.ds(at, STEP), :] += dot_nt(hit, facts)

            first = starts[8 * i + 4 * half, own]
            last = starts[jnp.minimum(8 * i + 4 * half + 4, ROWS - 1), own] + 16
            if half == 1:
                last = jnp.where(i == 7, total, last)
            rounds = (jnp.minimum(last, N1) - first + STEP - 1) // STEP
            add(pl.multiple_of(jnp.minimum(first, N1), 16))

            def more(k, carry, first=first, add=add):
                add(pl.multiple_of(first + STEP * k, 16))
                return carry

            lax.fori_loop(1, rounds, more, 0)
        return carry

    lax.fori_loop(0, 8, compact, 0)
    grid_copy.wait()
    T = 384
    lower = onehot(iota((T, T), 1) < iota((T, T), 0))

    def place(i, state):
        carry, bad = state
        at = pl.ds(pl.multiple_of(T * i, T), T)
        facts = meta[at, :]
        valid = facts[:, 5:6] > 0.5
        sender = jnp.where(valid, facts[:, 0:1] * 256.0 + facts[:, 1:2], -1.0)
        hit = onehot(iota((T, G), 1).astype(F32) == sender)
        sent_ref[at, :] = dot(hit, grid[...]).astype(BF)
        list_ref[at, :] = acc[at, :].astype(BF)
        lane = iota((T, 128), 1)
        info = jnp.where(lane == 0, facts[:, 3:4], jnp.where(lane == 1, facts[:, 4:5], 0.0))
        info_ref[at, :] = jnp.where(lane == 2, 1.0, info).astype(BF)
        owner = jnp.where((lane.astype(F32) == facts[:, 2:3]) & valid, 1.0, 0.0)
        rank = jnp.sum(owner * (dot(lower, owner.astype(BF)) + carry), axis=1, keepdims=True)
        carry = carry + jnp.sum(owner, axis=0, keepdims=True)
        d = facts[:, 2:3] - patch.astype(F32)
        d = jnp.where(d < 0.0, d + NP, d)
        more = rank - CA
        slot = jnp.where((d == 1.0) & (more < CX), OP + more, -1.0)
        slot = jnp.where((d == NP - 1.0) & (more < CX), OM + more, slot)
        slot = jnp.where(rank < CA, facts[:, 2:3] * CA + rank, slot)
        slot = jnp.where(d == 0.0, jnp.where(rank < CS, OS + rank, -1.0), slot)
        bad = jnp.maximum(bad, jnp.max(jnp.where(valid & (slot < 0.0), 1.0, 0.0)))
        slots = jnp.broadcast_to(jnp.where(valid, slot, -1.0), (T, 128))
        slot_ref[at, :] = slots[:, 0:8]
        slot_row_ref[:, at] = slots.T[0:8, :]
        return carry, bad

    bad = jnp.maximum(jnp.where(total > N1, 1.0, 0.0), spread)
    _, bad = lax.fori_loop(0, N1 // T, place, (jnp.zeros((1, 128), F32), bad))
    slot_row_ref[:, N1 : N1 + 128] = jnp.broadcast_to(bad, (8, 128))


def gather(count, where, receivers, mesh_slot, senders, edge_latent, grid_latent):
    sds = jax.ShapeDtypeStruct
    smem = pl.BlockSpec(memory_space=pltpu.SMEM)
    vmem = pl.BlockSpec(memory_space=pltpu.VMEM)
    hbm = pl.BlockSpec(memory_space=pl.ANY)
    return pl.pallas_call(
        gather_kernel,
        out_shape=(
            sds((ROWS, 128), F32), sds((ROWS + 8, 128), I32),
            sds((N1, D), BF), sds((N1, D), BF), sds((N1, 128), BF), sds((N1, 8), F32), sds((8, N1 + 128), F32),
            sds((ROWS, 128), F32),
        ),
        in_specs=[smem, smem, vmem, vmem, vmem, hbm, hbm],
        scratch_shapes=[
            pltpu.VMEM((640, 256), BF),
            pltpu.VMEM((1024, 640), BF),
            pltpu.VMEM((7, ROWS, 128), F32),
            pltpu.SMEM((ROWS + 8, 128), I32),
            pltpu.VMEM((E, D), BF),
            pltpu.VMEM((G, D), BF),
            pltpu.VMEM((N1 + STEP, D), F32),
            pltpu.VMEM((N1 + STEP, 8), F32),
            pltpu.SemaphoreType.DMA((8,)),
            pltpu.SemaphoreType.DMA(()),
            pltpu.SemaphoreType.DMA(()),
        ],
        compiler_params=pltpu.CompilerParams(vmem_limit_bytes=VMEM),
        name="gather",
    )(
        count, where, receivers.reshape(ROWS, 128), mesh_slot.reshape(640, 128), senders.reshape(ROWS, 128),
        edge_latent, grid_latent,
    )


def walk_of(own):
    x, core = own // 2, own % 2
    places = [2 * ((x + 4 - k) % 4) for k in range(4)]
    return [p + core for p in places] + [p + 1 - core for p in places]


def vectors_of(v_ref, m, order=tuple(range(NH))):
    pairs = []
    for k in range(NH // 2):
        at = slice(128 * m, 128 * m + 128)
        x, y = v_ref[order[2 * k], :, at].astype(F32), v_ref[order[2 * k + 1], :, at].astype(F32)
        pairs.append(lane_join(x, y))
    rows = [jnp.concatenate([p[i] for p in pairs], axis=1) for i in range(2)]
    return [r[0:1] + r[1:2] + r[2:3] for r in rows]


def stack_kernel(e, s, r, mi, mm, eo, mo, *refs):
    vectors, (first_ref, second_ref) = refs[:8], refs[8:]
    for k, w in enumerate((r, mi, mm, eo, mo)):
        second_ref[64 * k : 64 * k + 64, :] = w[...]
    v = jnp.concatenate([x[...] for x in vectors], axis=1)
    v = jnp.broadcast_to(v, (8, D))
    hi = v.astype(BF)
    v = v - hi.astype(F32)
    mid = v.astype(BF)
    low = (v - mid.astype(F32)).astype(BF)
    row = iota((8, D), 0)
    parts = jnp.where(row == 0, hi.astype(F32), jnp.where(row == 1, mid.astype(F32), low.astype(F32)))
    parts = jnp.where(row < 3, parts, 0.0).astype(BF)
    for n in range(NH):
        first_ref[n, 0:64, :] = e[...]
        first_ref[n, 64:128, :] = s[...]
        first_ref[n, VROW:WROWS, :] = parts


def stacked(*args):
    return pl.pallas_call(
        stack_kernel,
        out_shape=(jax.ShapeDtypeStruct((NH, WROWS, D), BF), jax.ShapeDtypeStruct((320, D), BF)),
        name="stacked",
    )(*args)


def to_all(first, second):
    first = lax.all_to_all(first, "hidden", split_axis=0, concat_axis=0, tiled=True)
    walk = [second]
    for k in (1, 2, 3):
        walk.append(lax.ppermute(second, "hidden", [(i, (i + 2 * k) % NH) for i in range(NH)]))
    walk = jnp.stack(walk)
    other = lax.ppermute(walk, "hidden", [(i, i ^ 1) for i in range(NH)])
    return first, walk, other


def pack_kernel(where_ref, list_ref, sent_ref, info_ref, slot_row_ref, first_ref, oa_ref, op_ref, om_ref, pre, wide):
    order = walk_of(where_ref[0])
    w_edge = jnp.concatenate([first_ref[n, 0:64, :] for n in order], axis=0)
    w_sender = jnp.concatenate([first_ref[n, 64:128, :] for n in order], axis=0)
    bias = vectors_of(first_ref.at[:, VROW:WROWS], 0, order)[0]
    T = 384
    for i in range(N1 // T):
        at = slice(T * i, T * i + T)
        pre[at, 0:D] = (dot_nt(list_ref[at, :], w_edge) + dot_nt(sent_ref[at, :], w_sender) + bias).astype(BF)
    pre[:, D : D + 128] = info_ref[...]

    def spread(i, carry):
        hit = onehot((iota((T, N1), 0) + T * i).astype(F32) == slot_row_ref[0:1, 0:N1])
        wide[pl.ds(pl.multiple_of(T * i, T), T), :] = dot(hit, pre[...])
        return carry

    lax.fori_loop(0, OS // T, spread, 0)
    kind = iota((8, 128), 0)
    bad = slot_row_ref[0:8, N1 : N1 + 128]

    def facts_of(at):
        return jnp.where(kind == 3, bad, wide[at : at + 128, D : D + 128].T[0:8, :])

    for i in range(NP // 2):
        x = facts_of(128 * i)
        low = iota((8, 128), 1) < 64
        turned = pltpu.roll(x, 64, 1)
        for odd in range(2):
            n = 2 * i + odd
            oa_ref[n, 0:CA, :] = wide[CA * n : CA * n + CA, 0:D].astype(BF)
            both = jnp.where(low, turned, x) if odd else jnp.where(low, x, turned)
            oa_ref[n, CA : CA + 8, :] = jnp.zeros((8, D), BF)
            oa_ref[n, CA : CA + 8, 0:128] = both.astype(BF)
    for ref, at, size in ((op_ref, OP, CX), (om_ref, OM, CX)):
        ref[0:size, :] = wide[at : at + size, 0:D].astype(BF)
        ref[size : size + 8, :] = jnp.zeros((8, D), BF)
        for k in range((size + 127) // 128):
            ref[size : size + 8, 128 * k : 128 * k + 128] = facts_of(at + 128 * k).astype(BF)


def pack(where, edges, sent, info, slot_row, first):
    sds = jax.ShapeDtypeStruct
    fixed = lambda *shape: pl.BlockSpec(shape, lambda b: (0,) * len(shape))
    shapes = ((NP, CA + 8, D), (CX + 8, D), (CX + 8, D), (N1, D + 128))
    return pl.pallas_call(
        pack_kernel,
        grid=(1,),
        in_specs=[pl.BlockSpec(memory_space=pltpu.SMEM)]
        + [fixed(N1, D), fixed(N1, D), fixed(N1, 128), fixed(8, N1 + 128), fixed(NH, WROWS, D)],
        out_specs=tuple(fixed(*x) for x in shapes),
        out_shape=tuple(sds(x, BF) for x in shapes),
        scratch_shapes=[pltpu.VMEM((OS, D + 128), F32)],
        compiler_params=pltpu.CompilerParams(vmem_limit_bytes=VMEM),
        name="pack",
    )(where, edges, sent, info, slot_row, first)


def full(w_refs):
    return jnp.concatenate([w[...].reshape(D // 2, D) for w in w_refs], axis=0)


def weight_specs(*which):
    one = lambda k: pl.BlockSpec((NH // 2, 64, D), lambda *_: (0, k, 0))
    vec = pl.BlockSpec((NH, 8, D), lambda *_: (0, VROW // 8, 0))
    return [one(k) for k in which for _ in range(2)] + [vec]


def messages(x, l, proj, w_out, vec):
    hit = onehot(iota((x.shape[0], ML), 1).astype(F32) == l)
    hidden = silu(x + dot(hit, proj)).astype(BF)
    message = normalized(dot(hidden, w_out) + vec[0], vec[1], vec[2])
    return jnp.where(l >= 0.0, message, 0.0).astype(BF)


def edge_vectors(v_ref):
    return vectors_of(v_ref, 1) + vectors_of(v_ref, 2)[0:1]


def local_kernel(where_ref, pre_ref, slot_row_ref, mesh_ref, wr_ref, wr2_ref, wo_ref, wo2_ref, v_ref, proj_ref, msg_ref, l_ref):
    proj = dot_nt(mesh_ref[...], full((wr_ref, wr2_ref))).astype(BF)
    proj_ref[...] = proj
    vec = edge_vectors(v_ref)
    w_out = full((wo_ref, wo2_ref))
    T = 128

    def some(i, carry):
        at = pl.ds(pl.multiple_of(T * i, T), T)
        hit = onehot((iota((T, N1), 0) + OS + T * i).astype(F32) == slot_row_ref[0:1, 0:N1])
        x = dot(hit, pre_ref[...])
        l = jnp.where(x[:, D + 2 : D + 3] > 0.5, x[:, D : D + 1] * 256.0 + x[:, D + 1 : D + 2], -1.0)
        msg_ref[at, :] = messages(x[:, 0:D], l, proj_ref[...], w_out, vec)
        l_ref[:, at] = jnp.broadcast_to(l, (T, 128)).T[0:8, :]
        return carry

    lax.fori_loop(0, CS // T, some, 0)


def local(where, pre, slot_row, mesh_latent, weights):
    first, walk, other = weights
    sds = jax.ShapeDtypeStruct
    fixed = lambda *shape: pl.BlockSpec(shape, lambda b, w: (0,) * len(shape))
    return pl.pallas_call(
        local_kernel,
        grid_spec=pltpu.PrefetchScalarGridSpec(
            num_scalar_prefetch=1,
            grid=(1,),
            in_specs=[
                fixed(N1, D + 128), fixed(8, N1 + 128),
                pl.BlockSpec((ML, D), lambda b, w: (w[0], 0)),
            ] + weight_specs(0, 3),
            out_specs=(fixed(ML, D), fixed(CS, D), fixed(8, CS)),
        ),
        out_shape=(sds((ML, D), BF), sds((CS, D), BF), sds((8, CS), F32)),
        compiler_params=pltpu.CompilerParams(vmem_limit_bytes=VMEM),
        name="local",
    )(where, pre, slot_row, mesh_latent, walk, other, walk, other, first)


def owner_kernel(
    ra_ref, rp_ref, rm_ref, proj_ref, wo_ref, wo2_ref, v_ref,
    oa_ref, op_ref, om_ref, l_row_ref, flag_ref,
    x_s, l_col,
):
    low = iota((8, 128), 1) < 64
    flags = jnp.zeros((8, 128), F32)
    pieces = []
    for i in range(NP // 2):
        a = ra_ref[2 * i, CA : CA + 8, 0:128].astype(F32)
        b = ra_ref[2 * i + 1, CA : CA + 8, 0:128].astype(F32)
        pieces.append(jnp.where(low, a, b))
    for ref, size in ((rp_ref, CX), (rm_ref, CX)):
        for k in range((size + 127) // 128):
            pieces.append(ref[size : size + 8, 128 * k : 128 * k + 128].astype(F32))
    for k, m in enumerate(pieces):
        flags = jnp.maximum(flags, m)
        l = jnp.where(m[2:3] > 0.5, m[0:1] * 256.0 + m[1:2], -1.0)
        l = jnp.broadcast_to(l, (8, 128))
        l_row_ref[:, 128 * k : 128 * k + 128] = l
        l_col[128 * k : 128 * k + 128, :] = l.T
    flag_ref[...] = jnp.broadcast_to(flags[3:4], (8, 128))
    for n in range(NP):
        x_s[CA * n : CA * n + CA, :] = ra_ref[n, 0:CA, :]
    for ref, at in ((rp_ref, OP), (rm_ref, OM)):
        x_s[at : at + CX, :] = ref[0:CX, :]
        x_s[at + CX : at + 256, :] = jnp.zeros((256 - CX, D), BF)
    vec = edge_vectors(v_ref)
    w_out = full((wo_ref, wo2_ref))
    T = 384

    def some(i, carry):
        at = pl.ds(pl.multiple_of(T * i, T), T)
        x_s[at, :] = messages(x_s[at, :].astype(F32), l_col[at, 0:1], proj_ref[...], w_out, vec)
        return carry

    lax.fori_loop(0, OS // T, some, 0)
    for n in range(NP):
        oa_ref[n, :, :] = x_s[CA * n : CA * n + CA, :]
    op_ref[...] = x_s[OP : OP + CX, :]
    om_ref[...] = x_s[OM : OM + CX, :]


def owner(ra, rp, rm, proj, weights):
    first, walk, other = weights
    sds = jax.ShapeDtypeStruct
    fixed = lambda *shape: pl.BlockSpec(shape, lambda b: (0,) * len(shape))
    return pl.pallas_call(
        owner_kernel,
        grid=(1,),
        in_specs=[fixed(NP, CA + 8, D), fixed(CX + 8, D), fixed(CX + 8, D), fixed(ML, D)] + weight_specs(3),
        out_specs=(fixed(NP, CA, D), fixed(CX, D), fixed(CX, D), fixed(8, OS), fixed(8, 128)),
        out_shape=(
            sds((NP, CA, D), BF), sds((CX, D), BF), sds((CX, D), BF), sds((8, OS), F32), sds((8, 128), F32),
        ),
        scratch_shapes=[pltpu.VMEM((OS, D), BF), pltpu.VMEM((OS, 8), F32)],
        compiler_params=pltpu.CompilerParams(vmem_limit_bytes=VMEM),
        name="owner",
    )(ra, rp, rm, proj, walk, other, first)


def nodes_kernel(
    where_ref, oa_ref, op_ref, om_ref, own_msg_ref, l_ref, own_l_ref, mesh_ref,
    wi_ref, wi2_ref, wm_ref, wm2_ref, wo_ref, wo2_ref, v_ref,
    out_ref, out_s,
):
    bias = vectors_of(v_ref, 0, walk_of(where_ref[0]))[1:2]
    vec = bias + vectors_of(v_ref, 2)[1:2] + vectors_of(v_ref, 3)
    w_in, w_msg, w_out = full((wi_ref, wi2_ref)), full((wm_ref, wm2_ref)), full((wo_ref, wo2_ref))
    S = ML // 4

    def some(i, carry):
        at = pl.ds(pl.multiple_of(S * i, S), S)
        row = (iota((S, 1), 0) + S * i).astype(F32)
        summed = dot(onehot(row == l_ref[0:1, 0:OP]), oa_ref[...].reshape(OP, D))
        summed += dot(onehot(row == l_ref[0:1, OP : OP + CX]), op_ref[...])
        summed += dot(onehot(row == l_ref[0:1, OM : OM + CX]), om_ref[...])
        summed += dot(onehot(row == own_l_ref[0:1, :]), own_msg_ref[...])
        own = mesh_ref[at, :]
        before = dot_nt(own, w_in) + dot_nt(summed.astype(BF), w_msg) + vec[0]
        hidden = silu(before).astype(BF)
        total = dot(hidden, w_out) + vec[1]
        out_s[at, :] = own.astype(F32) + normalized(total, vec[2], vec[3])
        return carry

    lax.fori_loop(0, 4, some, 0)
    for t in range(ML // 128):
        for k in range(4):
            turned = out_s[128 * t : 128 * t + 128, 128 * k : 128 * k + 128].T.astype(BF)
            out_ref[2 * k, 64 * t : 64 * t + 64, :] = turned[0:64]
            out_ref[2 * k + 1, 64 * t : 64 * t + 64, :] = turned[64:128]


def nodes(where, oa, op, om, own_msg, l_row, own_l, mesh_latent, weights):
    first, walk, other = weights
    sds = jax.ShapeDtypeStruct
    fixed = lambda *shape: pl.BlockSpec(shape, lambda b, w: (0,) * len(shape))
    return pl.pallas_call(
        nodes_kernel,
        grid_spec=pltpu.PrefetchScalarGridSpec(
            num_scalar_prefetch=1,
            grid=(1,),
            in_specs=[
                fixed(NP, CA, D), fixed(CX, D), fixed(CX, D), fixed(CS, D), fixed(8, OS), fixed(8, CS),
                pl.BlockSpec((ML, D), lambda b, w: (w[0], 0)),
            ] + weight_specs(1, 2, 4),
            out_specs=fixed(NH, ML // 2, 128),
            scratch_shapes=[pltpu.VMEM((ML, D), F32)],
        ),
        out_shape=sds((NH, ML // 2, 128), BF),
        compiler_params=pltpu.CompilerParams(vmem_limit_bytes=VMEM),
        name="nodes",
    )(where, oa, op, om, own_msg, l_row, own_l, mesh_latent, walk, other, walk, other, walk, other, first)


def unpack_kernel(ma_ref, mp_ref, mm_ref, ms_ref, slot_ref, flag_ref, mesh_ref, out_ref, msg, rows):
    for n in range(NP):
        msg[CA * n : CA * n + CA, :] = ma_ref[n]
    for ref, at in ((mp_ref, OP), (mm_ref, OM)):
        msg[at : at + CX, :] = ref[...]
        msg[at + CX : at + 256, :] = jnp.zeros((256 - CX, D), BF)
    msg[OS : OS + CS, :] = ms_ref[...]
    T = 384

    def one(i, carry):
        at = pl.ds(pl.multiple_of(T * i, T), T)
        hit = onehot(iota((T, NS), 1).astype(F32) == slot_ref[at, 0:1])
        rows[at, :] = dot(hit, msg[...])
        return carry

    lax.fori_loop(0, N1 // T, one, 0)
    for k in range(NH // 2):
        at = slice(128 * k, 128 * k + 128)
        a, b = lane_join(rows[0:HALF, at], rows[HALF:N1, at])
        out_ref[2 * k, 0:HALF, :] = a.astype(BF)
        out_ref[2 * k + 1, 0:HALF, :] = b.astype(BF)
    flag = jnp.concatenate([flag_ref[...]] * (FLAG // 8), axis=0).astype(BF)
    for n in range(NH):
        out_ref[n, HALF:MESH_AT, :] = flag
        out_ref[n, MESH_AT:OUT_ROWS, :] = mesh_ref[n]


def unpack(ma, mp, mm, ms, slots, flag, mesh_blocks):
    return pl.pallas_call(
        unpack_kernel,
        out_shape=jax.ShapeDtypeStruct((NH, OUT_ROWS, 128), BF),
        scratch_shapes=[pltpu.VMEM((NS, D), BF), pltpu.VMEM((N1, D), F32)],
        compiler_params=pltpu.CompilerParams(vmem_limit_bytes=VMEM),
        name="unpack",
    )(ma, mp, mm, ms, slots, flag, mesh_blocks)


def columns_kernel(where_ref, edge_ref, out_ref):
    odd = (where_ref[0] & 1) == 1
    low = iota((128, 128), 1) < 64
    for i in range(8):
        a = edge_ref[256 * i : 256 * i + 128, :].astype(F32)
        b = edge_ref[256 * i + 128 : 256 * i + 256, :].astype(F32)
        left, right = jnp.where(low, a, pltpu.roll(b, 64, 1)), jnp.where(low, pltpu.roll(a, 64, 1), b)
        turned = jnp.where(odd, right, left).T.astype(BF)
        out_ref[:, 256 * i : 256 * i + 128] = turned[0:64]
        out_ref[:, 256 * i + 128 : 256 * i + 256] = turned[64:128]


def columns(where, edge_latent):
    return pl.pallas_call(
        columns_kernel,
        grid_spec=pltpu.PrefetchScalarGridSpec(
            num_scalar_prefetch=1,
            grid=(4,),
            in_specs=[pl.BlockSpec((E // 4, 128), lambda b, w: (b, w[0] // 2))],
            out_specs=pl.BlockSpec((64, E // 4), lambda b, w: (0, b)),
        ),
        out_shape=jax.ShapeDtypeStruct((64, E), BF),
        compiler_params=pltpu.CompilerParams(vmem_limit_bytes=VMEM),
        name="columns",
    )(where, edge_latent)


def finish_kernel(starts_ref, in_ref, key_ref, column_ref, out_ref, mesh_ref, flag_ref, lists):
    flag = jnp.zeros((8, 128), F32)
    half = iota((HALF, 128), 1) < 64
    for n in range(NH):
        x = in_ref[n, 0:HALF, :].astype(F32)
        turned = pltpu.roll(x, 64, 1)
        lists[n, 0:HALF, :] = jnp.where(half, x, turned).astype(BF)
        lists[n, HALF:N1, :] = jnp.where(half, turned, x).astype(BF)
        lists[n, N1 : N1 + WIN, :] = jnp.zeros((WIN, 128), BF)
        flag = jnp.maximum(flag, in_ref[n, HALF : HALF + 8, :].astype(F32))
        for t in range(ML // 128):
            at = ML * n + 128 * t
            mesh_ref[:, at : at + 128] = in_ref[n, MESH_AT + 64 * t : MESH_AT + 64 * t + 64, :]
    flag_ref[0, 0] = (jnp.max(flag) > 0.5).astype(I32)
    low = iota((128, 128), 1) < 64
    lane = iota((128, NH * WIN), 1).astype(F32)

    def group(g, carry):
        key = key_ref[pl.ds(pl.multiple_of(8 * g, 8), 8), :]
        h = jnp.floor(key * (1.0 / 256.0))
        delta = key - 256.0 * h
        column = jnp.where((h >= 0.0) & (delta < WIN), h * WIN + delta, -1.0).T
        for i in range(4):
            sides = []
            for j in (2 * i, 2 * i + 1):
                hit = onehot(lane == column[:, j : j + 1])
                parts = []
                for n in range(NH):
                    at = jnp.minimum(starts_ref[8 * g + j, n], N1)
                    parts.append(lists[n, pl.ds(pl.multiple_of(at, 16), WIN), :])
                sides.append(dot(hit, jnp.concatenate(parts, axis=0)))
            turned = jnp.where(low, sides[0], sides[1]).T
            for k in range(2):
                at = pl.ds(pl.multiple_of(1024 * g + 256 * i + 128 * k, 128), 128)
                out_ref[:, at] = (turned[64 * k : 64 * k + 64] + column_ref[:, at].astype(F32)).astype(BF)
        return carry

    lax.fori_loop(0, 8, group, 0)


def finish(starts, lists, key, column):
    sds = jax.ShapeDtypeStruct
    smem = pl.BlockSpec(memory_space=pltpu.SMEM)
    vmem = pl.BlockSpec(memory_space=pltpu.VMEM)
    return pl.pallas_call(
        finish_kernel,
        in_specs=[smem, vmem, vmem, vmem],
        out_specs=(vmem, vmem, smem),
        out_shape=(sds((64, E), BF), sds((64, M), BF), sds((1, 1), I32)),
        scratch_shapes=[pltpu.VMEM((NH, N1 + WIN, 128), BF)],
        compiler_params=pltpu.CompilerParams(vmem_limit_bytes=VMEM),
        name="finish",
    )(starts, lists, key, column)


def exchange(a, p, m, away):
    up = [(i, (i + 1) % NP) for i in range(NP)]
    down = [(i, (i - 1) % NP) for i in range(NP)]
    first, second = (up, down) if away else (down, up)
    p = lax.ppermute(p, "patch", first)
    m = lax.ppermute(m, "patch", second)
    a = lax.all_to_all(a, "patch", split_axis=0, concat_axis=0, tiled=True)
    return a, p, m


def fast(
    grid_latent, mesh_latent, edge_latent, senders, receivers, mesh_slot, edge_counts,
    w_edge, w_sender, w_receiver, edge_bias, w_edge_out, edge_out_bias, edge_gain, edge_shift,
    w_mesh_in, w_message_in, mesh_bias, w_mesh_out, mesh_out_bias, mesh_gain, mesh_shift,
):
    patch = lax.axis_index("patch").astype(I32)
    own = lax.axis_index("hidden").astype(I32)
    where = jnp.stack([own, patch])
    vectors = (edge_bias, mesh_bias, edge_out_bias, edge_gain, edge_shift, mesh_out_bias, mesh_gain, mesh_shift)
    first, second = stacked(
        w_edge.T, w_sender.T, w_receiver.T, w_mesh_in.T, w_message_in.T, w_edge_out, w_mesh_out,
        *(v.reshape(1, 64) for v in vectors),
    )
    weights = to_all(first, second)
    key, starts, edges, sent, info, slots, slot_row, target = gather(
        edge_counts, where, receivers, mesh_slot, senders, edge_latent, grid_latent
    )
    sa, sp, sm, pre = pack(where, edges, sent, info, slot_row, weights[0])
    ra, rp, rm = exchange(sa, sp, sm, True)
    proj, ms, own_l = local(where, pre, slot_row, mesh_latent, weights)
    column = columns(where, edge_latent)
    oa, op, om, l_row, flag = owner(ra, rp, rm, proj, weights)
    ma, mp, mm = exchange(oa, op, om, False)
    mesh_blocks = nodes(where, oa, op, om, ms, l_row, own_l, mesh_latent, weights)
    lists = unpack(ma, mp, mm, ms, slots, flag, mesh_blocks)
    lists = lax.all_to_all(lists, "hidden", split_axis=0, concat_axis=0, tiled=True)
    edge_out, mesh_out, flag = finish(starts, lists, key, column)
    return mesh_out.T, edge_out.T, flag, target


def from_everyone(x):
    copies = jnp.broadcast_to(x, (NH, *x.shape))
    return lax.all_to_all(copies, "hidden", split_axis=0, concat_axis=0, tiled=True)


def by_rows(f, size, *xs):
    part = lambda x, i: lax.dynamic_slice_in_dim(x, size * i, size)
    shape = jax.eval_shape(f, *(jax.ShapeDtypeStruct((size, *x.shape[1:]), x.dtype) for x in xs))
    out = jnp.zeros((xs[0].shape[0], *shape.shape[1:]), shape.dtype)

    def one(i, out):
        return lax.dynamic_update_slice_in_dim(out, f(*(part(x, i) for x in xs)), size * i, 0)

    return lax.fori_loop(0, xs[0].shape[0] // size, one, out)


def times(x, w):
    return by_rows(lambda y: dot(y, w), 128, x)


def rows_at(table, index):
    ids = jnp.arange(table.shape[0], dtype=I32)
    return by_rows(lambda at: dot((at[:, None] == ids[None, :]).astype(BF), table), 128, index)


def sums_at(rows, index):
    def some(ids):
        def one(i, out):
            at = lax.dynamic_slice_in_dim(index, 512 * i, 512)
            return out + dot((ids[:, None] == at[None, :]).astype(BF), lax.dynamic_slice_in_dim(rows, 512 * i, 512))

        return lax.fori_loop(0, E // 512, one, jnp.zeros((ids.shape[0], rows.shape[1]), F32))

    return by_rows(some, 128, jnp.arange(M, dtype=I32))


def second_layer(pre, w):
    partial = by_rows(lambda x: dot(silu(x).astype(BF), w).astype(BF), 128, pre)
    blocks = lax.all_to_all(jnp.stack(jnp.split(partial, NH, axis=1)), "hidden", split_axis=0, concat_axis=0, tiled=True)
    return by_rows(lambda *x: sum(y.astype(F32) for y in x), 128, *blocks)


def finished(v, gain, shift, scale, columns):
    parts = by_rows(lambda x: jnp.stack([jnp.sum(x, axis=1), jnp.sum(x * x, axis=1)], axis=1), 128, v)
    total = from_everyone(parts.T).sum(axis=0).T / D

    def one(x, t, scale):
        var = jnp.maximum(t[:, 1:2] - t[:, 0:1] * t[:, 0:1], 0.0)
        return ((x - t[:, 0:1]) * lax.rsqrt(var + EPSILON) * gain + shift) * scale

    change = by_rows(one, 128, v, total, scale)
    return by_rows(lambda c, x: (c.astype(F32) + x).astype(BF), 128, columns, change), change


def slow(
    target,
    grid_latent, mesh_latent, edge_latent, senders, receivers, mesh_slot, edge_counts,
    w_edge, w_sender, w_receiver, edge_bias, w_edge_out, edge_out_bias, edge_gain, edge_shift,
    w_mesh_in, w_message_in, mesh_bias, w_mesh_out, mesh_out_bias, mesh_gain, mesh_shift,
):
    patch = lax.axis_index("patch").astype(I32)
    own = lax.axis_index("hidden").astype(I32)
    up = [(i, (i + 1) % NP) for i in range(NP)]
    target = target.astype(I32).reshape(E)
    whose = target // M
    local = target - whose * M
    live = (jnp.arange(E, dtype=I32) < edge_counts[0]).astype(F32)
    sent = rows_at(grid_latent, senders - patch * G).astype(BF)
    pre = times(edge_latent, w_edge) + times(sent, w_sender) + edge_bias

    def fetch(s, state):
        block, pre = state
        pre = pre + rows_at(block, jnp.where(whose == (patch - s) % NP, local, -1))
        return lax.ppermute(block, "patch", up), pre

    block = times(mesh_latent, w_receiver).astype(BF)
    _, pre = lax.fori_loop(0, NP, fetch, (block, pre))
    total = second_layer(pre, w_edge_out) + edge_out_bias
    columns = lax.dynamic_slice_in_dim(edge_latent, own * 64, 64, 1)
    edge_out, message = finished(total, edge_gain, edge_shift, live[:, None], columns)
    rows = message.astype(BF)

    def collect(s, sums):
        part = sums_at(rows, jnp.where(whose == (patch - 1 - s) % NP, local, -1))
        return lax.ppermute(sums, "patch", up) + part

    sums = lax.fori_loop(0, NP, collect, jnp.zeros((M, 64), F32))
    summed = jnp.concatenate(list(from_everyone(sums.astype(BF))), axis=1)
    before = times(mesh_latent, w_mesh_in) + times(summed, w_message_in) + mesh_bias
    total = second_layer(before, w_mesh_out) + mesh_out_bias
    columns = lax.dynamic_slice_in_dim(mesh_latent, own * 64, 64, 1)
    mesh_out, _ = finished(total, mesh_gain, mesh_shift, jnp.ones((M, 1), F32), columns)
    return mesh_out, edge_out


def shards(*args):
    mesh_out, edge_out, flag, target = fast(*args)
    return lax.cond(
        flag[0, 0] > 0, lambda a, done: slow(*a), lambda a, done: done, (target, *args), (mesh_out, edge_out)
    )


def solution(mesh):
    rows, columns, units = P("patch", None), P(None, "hidden"), P("hidden")
    return jax.shard_map(
        shards,
        mesh=mesh,
        in_specs=(
            rows, rows, rows, P("patch"), P("patch"), P(), P("patch"),
            columns, columns, columns, units, P("hidden", None), units, units, units,
            columns, columns, units, P("hidden", None), units, units, units,
        ),
        out_specs=(P("patch", "hidden"), P("patch", "hidden")),
        check_vma=False,
    )
```
